32 devices in a mesh: dp: 8 (over y, x, core), expert: 4 (over z).
Axes of the slice: x: 2, y: 2, z: 4, core: 2. Of those that a mesh axis runs over, the one named last changes fastest.
Arguments:
- images: bfloat16 [2, 32, 197, 512], P(None, ('dp', 'expert')), may hold values from -6 to 6
- cotangent: bfloat16 [2, 32, 197, 512], P(None, ('dp', 'expert')), may hold values from -6 to 6
- gates: float32 [2, 32, 197, 2], P(None, ('dp', 'expert')), may hold values from 0.2 to 1
- routes: int32 [2, 32, 197, 2], P(None, ('dp', 'expert')), may hold values from 0 to 3, as said below
- slots: int32 [2, 32, 197, 2], P(None, ('dp', 'expert')), may hold values from 0 to 196, as said below
- dense_master: float32 [2048, 512], P('dp')
- dense_momentum: float32 [2048, 512], P('dp'), may hold values from -256 to 256
- norm_master: float32 [4, 512], P(None, 'dp')
- norm_momentum: float32 [4, 512], P(None, 'dp'), may hold values from -320 to 320
- expert_master: float32 [4, 2, 2048, 512], P('expert', None, 'dp')
- expert_momentum: float32 [4, 2, 2048, 512], P('expert', None, 'dp'), may hold values from -128 to 128
Outputs:
- activations: bfloat16 [2, 32, 197, 512], P(None, ('dp', 'expert'))
- input_grad: bfloat16 [2, 32, 197, 512], P(None, ('dp', 'expert'))
- dense_grad: float32 [2048, 512], P('dp')
- norm_grad: float32 [4, 512], P(None, 'dp')
- expert_grad: float32 [4, 2, 2048, 512], P('expert', None, 'dp')
- dense_moment: float32 [2048, 512], P('dp')
- norm_moment: float32 [4, 512], P(None, 'dp')
- expert_moment: float32 [4, 2, 2048, 512], P('expert', None, 'dp')
- dense_new: float32 [2048, 512], P('dp')
- norm_new: float32 [4, 512], P(None, 'dp')
- expert_new: float32 [4, 2, 2048, 512], P('expert', None, 'dp')
- dense_copy: bfloat16 [2048, 512], P('dp')
- expert_copy: bfloat16 [4, 2, 2048, 512], P('expert', None, 'dp')
The draws below stay inside these ranges and needn't reach their ends.
Inputs may be any that keep to these rules, and one draw needn't show every extreme that they name: Within each micro-batch and each block of 1 images, a token's two routes differ and no expert is named by more than 197 routes; every expert is named in every block; in each micro-batch, in every run of 4 consecutive blocks that starts at a multiple of 4, some expert is named exactly 197 times in each block. Within a block, the routes to one expert have the slots 0 to their number minus 1, each once.
All inputs are finite; a program needn't handle non-finite values.
Results may differ from the reference program's by a relative error of at most 0.025.
Values may be sent and summed in bfloat16 or wider, within the bound.
A program may use at most 192 MiB of HBM per device.

```python
from functools import partial
import jax
import jax.numpy as jnp
from jax import lax

D = 512
HEADS = 8
HDIM = 64
FF = 2048
SEQ = 197
MICRO = 2
IMG_MB = 1
EXPERTS = 4
CAP = 197
IMAGES_MB = 32
TOKENS = 12608


def route_plan(key):
    device_count = IMAGES_MB // IMG_MB
    rows = IMG_MB * SEQ
    busy = max(1, EXPERTS // 4)
    remaining = 2 * rows - busy * CAP
    light = remaining // (EXPERTS - busy)
    extra = remaining % (EXPERTS - busy)
    ranks = jnp.arange(EXPERTS, dtype=jnp.int32)
    counts = jnp.where(ranks < busy, CAP, light + (ranks - busy < extra).astype(jnp.int32)).astype(jnp.int32)
    starts = jnp.cumsum(counts) - counts
    entries = jnp.arange(2 * rows, dtype=jnp.int32)
    entry_rank = jnp.sum((entries[:, None] >= starts[None, :]).astype(jnp.int32), axis=1) - 1
    entry_slot = entries - starts[entry_rank]
    group_base = jax.random.fold_in(key, 3)
    token_base = jax.random.fold_in(key, 7)

    def one_block(block):
        micro = block // device_count
        device = block % device_count
        order = jax.random.permutation(jax.random.fold_in(group_base, micro * device_count + device // EXPERTS), EXPERTS).astype(jnp.int32)
        tokens = jax.random.permutation(jax.random.fold_in(token_base, block), rows).astype(jnp.int32)
        expert_of = order[entry_rank]
        pair = jnp.stack([expert_of[:rows], expert_of[rows:]], axis=1)
        pair_slot = jnp.stack([entry_slot[:rows], entry_slot[rows:]], axis=1)
        routes_block = jnp.zeros((rows, 2), jnp.int32).at[tokens].set(pair)
        slots_block = jnp.zeros((rows, 2), jnp.int32).at[tokens].set(pair_slot)
        return (routes_block, slots_block)
    routes_all, slots_all = jax.vmap(one_block)(jnp.arange(MICRO * device_count, dtype=jnp.int32))
    shape = (MICRO, IMAGES_MB, SEQ, 2)
    return (routes_all.reshape(shape), slots_all.reshape(shape))


def draw_routes(key, part):
    return route_plan(key)[0]


def draw_slots(key, part):
    return route_plan(key)[1]


def base_noise(key, shape):
    return jax.random.normal(key, shape, jnp.float32)


def draw_dense_master(key, part):
    noise = base_noise(key, (4 * D, D))
    row_index = jnp.arange(4 * D)[:, None]
    spread = jnp.where(row_index < 2 * D, 1.4 * float(D) ** (-0.5), 1.6 * float(D) ** (-0.5))
    return (noise * spread).astype(jnp.float32)


def draw_norm_master(key, part):
    noise = base_noise(key, (4, D))
    row_index = jnp.arange(4)[:, None]
    return jnp.where(row_index % 2 == 0, 1.0 + 0.1 * noise, 0.3 * noise).astype(jnp.float32)


def draw_expert_master(key, part):
    noise = base_noise(key, (EXPERTS, 2, FF, D))
    which = jnp.arange(2)[None, :, None, None]
    spread = jnp.where(which == 0, float(D) ** (-0.5), float(FF) ** (-0.5))
    return (noise * spread).astype(jnp.float32)


def shard_levels(own_key, dims, pieces, low, largest):
    def one(dim, blocks):
        heights = jax.random.uniform(jax.random.fold_in(jax.random.fold_in(own_key, 6), dim), (blocks,), jnp.float32, low / len(pieces), largest / len(pieces))
        return jnp.repeat(jnp.exp(heights), dims[dim] // blocks).reshape((-1,) + (1,) * (len(dims) - dim - 1))

    loudness = one(*pieces[0])
    for cut in pieces[1:]:
        loudness = loudness * one(*cut)
    return loudness


def scatter_about(key, dims, deviation, most, cuts=(), kind=jnp.bfloat16):
    drawn = jax.random.normal(key, dims, jnp.float32) * deviation
    if len(cuts) > 0:
        drawn = shard_levels(key, dims, cuts, -0.22, 0.18) * drawn
    return jnp.clip(drawn, min=-most, max=most).astype(kind)


def setup_inputs(seed: int = 0) -> dict:
    keys = jax.random.split(jax.random.key(seed), 12)
    images = scatter_about(keys[0], (MICRO, IMAGES_MB, SEQ, D), 1.0, 6.0, ((1, 32),))
    cotangent = scatter_about(keys[1], (MICRO, IMAGES_MB, SEQ, D), 1.0, 6.0, ((1, 32),))
    gates = jnp.clip(0.2 + 0.8 * jax.random.uniform(keys[2], (MICRO, IMAGES_MB, SEQ, 2), jnp.float32) ** shard_levels(keys[2], (MICRO, IMAGES_MB, SEQ, 2), ((1, 32),), -0.2, 0.2), 0.2, 1.0)
    routes = draw_routes(jax.random.fold_in(keys[11], 71), 0)
    slots = draw_slots(jax.random.fold_in(keys[11], 71), 0)
    dense_master = draw_dense_master(jax.random.fold_in(keys[11], 71), 0)
    dense_momentum = scatter_about(keys[6], (4 * D, D), (0.4 * TOKENS ** 0.5), 256.0, ((0, 8),), jnp.float32)
    norm_master = draw_norm_master(jax.random.fold_in(keys[11], 71), 0)
    norm_momentum = scatter_about(keys[8], (4, D), (0.5 * TOKENS ** 0.5), 320.0, ((1, 8),), jnp.float32)
    expert_master = draw_expert_master(jax.random.fold_in(keys[11], 71), 0)
    expert_momentum = scatter_about(keys[10], (EXPERTS, 2, FF, D), (0.3 * (2 * TOKENS // EXPERTS) ** 0.5), 128.0, ((0, 4), (2, 8)), jnp.float32)
    return {"images": images, "cotangent": cotangent, "gates": gates, "routes": routes, "slots": slots, "dense_master": dense_master, "dense_momentum": dense_momentum, "norm_master": norm_master, "norm_momentum": norm_momentum, "expert_master": expert_master, "expert_momentum": expert_momentum}


@jax.custom_vjp
def low(v):
    return lax.optimization_barrier(v.astype(jnp.bfloat16)).astype(jnp.float32)

@jax.custom_vjp
def low_back(v):
    return v

def low_keep(v):
    return (low(v), None)

def low_pass(kept, grad):
    return (grad,)

def back_keep(v):
    return (v, None)

def back_low(kept, grad):
    return (low(grad),)
low.defvjp(low_keep, low_pass)
low_back.defvjp(back_keep, back_low)
HIGH = lax.Precision.HIGHEST
NORM_EPS = 1e-06
ORTHO_EPS = 1e-07
NS_A = 3.4445
NS_B = -4.775
NS_C = 2.0315
DECAY = 0.5
LR_QKV = 0.5
LR_OUT = 1.5
LR_EXPERT = 0.5
LR_VECTOR = 0.05

def layer_norm(rows, norm_gain, norm_bias):
    row_mean = lax.optimization_barrier(jnp.mean(rows, axis=-1, keepdims=True))
    centred = rows - row_mean
    variance = lax.optimization_barrier(jnp.mean(centred * centred, axis=-1, keepdims=True))
    return centred * lax.rsqrt(variance + NORM_EPS) * norm_gain + norm_bias

def attend(normed_image, w_qkv, w_out):
    projected = low_back(low(jnp.dot(normed_image, w_qkv.T, precision=HIGH)))
    parts = projected.reshape(SEQ, 3, HEADS, HDIM)
    scores = low_back(jnp.einsum('qhd,khd->hqk', parts[:, 0], parts[:, 1], precision=HIGH) * HDIM ** (-0.5))
    soft_low = low(jax.nn.softmax(scores, axis=-1))
    mixed = low_back(low(jnp.einsum('hqk,khd->qhd', soft_low, parts[:, 2], precision=HIGH))).reshape(SEQ, D)
    return low_back(jnp.dot(mixed, w_out.T, precision=HIGH))

def place(rows_block, index_block):
    doubled = jnp.repeat(rows_block, 2, axis=0)
    return jnp.zeros((EXPERTS * CAP, D), rows_block.dtype).at[index_block].set(doubled)

def expert_apply(operands):
    buffer_rows, up_rows, down_rows = operands
    pre = low_back(jnp.dot(buffer_rows, up_rows.T, precision=HIGH))
    hidden = low(jax.nn.gelu(pre, approximate=False))
    return low_back(low(jnp.dot(hidden, down_rows, precision=HIGH)))

def forward(image_vals, dense_vals, norm_vals, expert_vals, gates, routes, slots):
    dense = low(dense_vals)
    norms = low(norm_vals)
    experts = low(expert_vals)
    w_qkv = dense[:3 * D]
    w_out = dense[3 * D:]
    stacked = image_vals.reshape(MICRO * IMAGES_MB, SEQ, D)
    normed_one = low(layer_norm(stacked, norms[0], norms[1]))
    branch = lax.map(jax.checkpoint(partial(attend, w_qkv=w_qkv, w_out=w_out)), normed_one)
    residual = stacked + branch
    normed_two = low(layer_norm(residual, norms[2], norms[3]))
    block_count = MICRO * (IMAGES_MB // IMG_MB)
    rows_block = IMG_MB * SEQ
    block_rows = normed_two.reshape(block_count, rows_block, D)
    flat_index = (routes * CAP + slots).reshape(block_count, 2 * rows_block).astype(jnp.int32)
    buffers = low_back(jax.vmap(place)(block_rows, flat_index))
    by_expert = buffers.reshape(block_count, EXPERTS, CAP, D).transpose(1, 0, 2, 3).reshape(EXPERTS, block_count * CAP, D)
    produced = lax.map(jax.checkpoint(expert_apply), (by_expert, experts[:, 0], experts[:, 1]))
    by_block = produced.reshape(EXPERTS, block_count, CAP, D).transpose(1, 0, 2, 3).reshape(block_count, EXPERTS * CAP, D)
    taken = jnp.take_along_axis(by_block, flat_index[:, :, None], axis=1).reshape(block_count, rows_block, 2, D)
    pair_gates = gates.reshape(block_count, rows_block, 2)
    moe = pair_gates[:, :, 0:1] * taken[:, :, 0] + pair_gates[:, :, 1:2] * taken[:, :, 1]
    return residual + moe.reshape(MICRO * IMAGES_MB, SEQ, D)

def orthogonalize(moment):
    current = moment / (jnp.sqrt(jnp.sum(moment * moment)) + ORTHO_EPS)
    for turn in range(5):
        gram = jnp.dot(current.T, current, precision=HIGH)
        blend = NS_B * gram + NS_C * jnp.dot(gram, gram, precision=HIGH)
        current = NS_A * current + jnp.dot(current, blend, precision=HIGH)
    return current

def reference(images, cotangent, gates, routes, slots, dense_master, dense_momentum, norm_master, norm_momentum, expert_master, expert_momentum):
    images_wide = images.astype(jnp.float32)

    def closed(image_vals, dense_vals, norm_vals, expert_vals):
        return forward(image_vals, dense_vals, norm_vals, expert_vals, gates, routes, slots)
    output, pull = jax.vjp(closed, images_wide, dense_master, norm_master, expert_master)
    grad_images, dense_grad, norm_grad, expert_grad = pull(cotangent.astype(jnp.float32).reshape(output.shape))
    dense_moment = DECAY * dense_momentum + dense_grad
    norm_moment = DECAY * norm_momentum + norm_grad
    expert_moment = DECAY * expert_momentum + expert_grad
    dense_step = jnp.concatenate([LR_QKV * orthogonalize(dense_moment[:3 * D]), LR_OUT * orthogonalize(dense_moment[3 * D:])], axis=0)
    dense_new = dense_master - dense_step
    norm_new = norm_master - LR_VECTOR * TOKENS ** (-0.5) * norm_moment
    expert_new = expert_master - LR_EXPERT * jax.vmap(jax.vmap(orthogonalize))(expert_moment)
    shape = (MICRO, IMAGES_MB, SEQ, D)
    return (output.reshape(shape).astype(jnp.bfloat16), grad_images.reshape(shape).astype(jnp.bfloat16), dense_grad, norm_grad, expert_grad, dense_moment, norm_moment, expert_moment, dense_new, norm_new, expert_new, dense_new.astype(jnp.bfloat16), expert_new.astype(jnp.bfloat16))
```

```python
from functools import partial

import jax
import jax.numpy as jnp
from jax import lax
from jax.experimental import pallas as pl
from jax.experimental.pallas import tpu as pltpu
from jax.sharding import PartitionSpec as P

MESH = pl.DeviceIdType.MESH
NT = (((1,), (1,)), ((), ()))

HEADS = 8


HIGH = lax.Precision.HIGHEST
NORM_EPS = 1e-06
ORTHO_EPS = 1e-07
NS_A = 3.4445
NS_B = -4.775
NS_C = 2.0315
DECAY = 0.5
LR_QKV = 0.5
LR_OUT = 1.5
LR_EXPERT = 0.5
LR_VECTOR = 0.05


def layer_norm(rows, norm_gain, norm_bias):
    row_mean = jnp.mean(rows, axis=-1, keepdims=True)
    centred = rows - row_mean
    variance = jnp.mean(centred * centred, axis=-1, keepdims=True)
    inverse = lax.rsqrt(variance + NORM_EPS)
    normed = centred * inverse
    return (normed * norm_gain + norm_bias, normed, inverse)


def norm_backward(grad_out, normed, inverse, norm_gain):
    grad_gain = jnp.sum(grad_out * normed, axis=0)
    grad_bias = jnp.sum(grad_out, axis=0)
    scaled = grad_out * norm_gain
    grad_rows = inverse * (
        scaled
        - jnp.mean(scaled, axis=-1, keepdims=True)
        - normed * jnp.mean(scaled * normed, axis=-1, keepdims=True)
    )
    return (grad_rows, grad_gain, grad_bias)


def split_heads(projected, heads):
    images_here, seq, triple = projected.shape
    head_size = triple // (3 * heads)
    parts = projected.reshape(images_here, seq, 3, heads, head_size)
    return (parts[:, :, 0], parts[:, :, 1], parts[:, :, 2], head_size ** (-0.5))


def attention_forward(normed_low, w_qkv, w_out, heads):
    images_here, seq, width = normed_low.shape
    projected = jnp.einsum(
        "bsd,ed->bse", normed_low, w_qkv, preferred_element_type=jnp.float32
    ).astype(jnp.bfloat16)
    query_part, key_part, value_part, score_scale = split_heads(projected, heads)
    scores = (
        jnp.einsum("bqhd,bkhd->bhqk", query_part, key_part, preferred_element_type=jnp.float32)
        * score_scale
    )
    top = jnp.max(scores, axis=-1, keepdims=True)
    expo = jnp.exp(scores - top)
    total = jnp.sum(expo, axis=-1, keepdims=True)
    soft_weights = expo / total
    log_total = top + jnp.log(total)
    mixed = jnp.einsum(
        "bhqk,bkhd->bqhd",
        soft_weights.astype(jnp.bfloat16),
        value_part,
        preferred_element_type=jnp.float32,
    )
    mixed = mixed.astype(jnp.bfloat16).reshape(images_here, seq, width)
    branch = jnp.einsum("bsd,ed->bse", mixed, w_out, preferred_element_type=jnp.float32)
    return (branch, (projected, log_total, mixed))


def attention_backward(grad_branch, normed_low, w_qkv, w_out, kept, heads):
    projected, log_total, mixed = kept
    images_here, seq, width = normed_low.shape
    query_part, key_part, value_part, score_scale = split_heads(projected, heads)
    grad_low = grad_branch.astype(jnp.bfloat16)
    grad_out_w = jnp.einsum("bse,bsd->ed", grad_low, mixed, preferred_element_type=jnp.float32)
    grad_mixed = jnp.einsum(
        "bse,ed->bsd", grad_low, w_out, preferred_element_type=jnp.float32
    ).astype(jnp.bfloat16)
    grad_mixed = grad_mixed.reshape(query_part.shape)
    scores = (
        jnp.einsum("bqhd,bkhd->bhqk", query_part, key_part, preferred_element_type=jnp.float32)
        * score_scale
    )
    soft_weights = jnp.exp(scores - log_total)
    soft_low = soft_weights.astype(jnp.bfloat16)
    grad_soft = jnp.einsum(
        "bqhd,bkhd->bhqk", grad_mixed, value_part, preferred_element_type=jnp.float32
    )
    grad_scores = (
        soft_weights * (grad_soft - jnp.sum(soft_weights * grad_soft, axis=-1, keepdims=True))
    ).astype(jnp.bfloat16)
    grad_query = (
        jnp.einsum("bhqk,bkhd->bqhd", grad_scores, key_part, preferred_element_type=jnp.float32)
        * score_scale
    )
    grad_key = (
        jnp.einsum("bhqk,bqhd->bkhd", grad_scores, query_part, preferred_element_type=jnp.float32)
        * score_scale
    )
    grad_value = jnp.einsum(
        "bhqk,bqhd->bkhd", soft_low, grad_mixed, preferred_element_type=jnp.float32
    )
    grad_projected = (
        jnp.stack([grad_query, grad_key, grad_value], axis=2)
        .reshape(images_here, seq, 3 * width)
        .astype(jnp.bfloat16)
    )
    grad_qkv_w = jnp.einsum(
        "bse,bsd->ed", grad_projected, normed_low, preferred_element_type=jnp.float32
    )
    grad_normed = jnp.einsum(
        "bse,ed->bsd", grad_projected, w_qkv, preferred_element_type=jnp.float32
    )
    return (grad_normed, grad_qkv_w, grad_out_w)


def muon_kernel(
    n_dp, width, expert_grad, dense_grad, expert_momentum, dense_momentum, expert_master,
    dense_master, expert_moment, dense_moment, expert_new, dense_new, expert_copy, dense_copy,
    outgoing, held, wide, low, blend, back, send_sem, take_sem, return_sem, back_sem,
):
    me = lax.axis_index("dp")
    rows = dense_grad.shape[0]
    turned = rows % 128 == 0

    def turn_over(block):
        return block.T if turned else block

    def slot(ref, place):
        where = pl.ds(pl.multiple_of(place * rows, rows), rows)
        return ref.at[:, where] if turned else ref.at[where, :]

    query_devices = 3 * width // rows
    own_up, own_down, own_query, own_out = 0, 3 * n_dp // 4, n_dp // 4, n_dp // 2
    dense_owner = jnp.where(me < query_devices, own_query, own_out)
    dense_place = jnp.where(me < query_devices, me, me - query_devices)
    barrier = pltpu.get_barrier_semaphore()
    for step in range(1, n_dp):
        pl.semaphore_signal(
            barrier, inc=1, device_id={"dp": lax.rem(me + step, n_dp)}, device_id_type=MESH
        )
    for job in range(2):
        moment = DECAY * expert_momentum[0, job] + expert_grad[0, job]
        expert_moment[0, job] = moment
        outgoing[job] = turn_over(moment.astype(jnp.bfloat16))
    moment = DECAY * dense_momentum[...] + dense_grad[...]
    dense_moment[...] = moment
    outgoing[2] = turn_over(moment.astype(jnp.bfloat16))
    pl.semaphore_wait(barrier, n_dp - 1)

    owners = (own_up, own_down, dense_owner)
    places = (me, me, dense_place)
    for job in range(3):
        @pl.when(me != owners[job])
        def _():
            pltpu.make_async_remote_copy(
                src_ref=outgoing.at[job], dst_ref=slot(held, places[job]),
                send_sem=send_sem.at[job], recv_sem=take_sem.at[me],
                device_id={"dp": owners[job]}, device_id_type=MESH,
            ).start()

        @pl.when(me == owners[job])
        def _():
            slot(held, places[job])[...] = outgoing[job]

    def take(source):
        @pl.when(me != source)
        def _():
            pltpu.make_async_remote_copy(
                src_ref=outgoing.at[0], dst_ref=slot(held, 0),
                send_sem=send_sem.at[0], recv_sem=take_sem.at[source],
                device_id={"dp": source}, device_id_type=MESH,
            ).wait_recv()

    query_rows = 3 * width
    out_rows = n_dp * rows - query_rows
    total = n_dp * rows

    def clear(first):
        zeros = jnp.zeros((total - first, width), jnp.bfloat16)
        if turned:
            held[:, first:] = zeros.T
        else:
            held[first:, :] = zeros

    def columns(start):
        where = slice(start, start + width)
        return (held[:, where] if turned else held[where, :].T).astype(jnp.float32)

    @pl.when((me == own_up) | (me == own_down))
    def _():
        for source in range(n_dp):
            take(source)

    @pl.when(me == own_query)
    def _():
        clear(query_rows)
        for source in range(query_devices):
            take(source)

    @pl.when(me == own_out)
    def _():
        clear(out_rows)
        for source in range(query_devices, n_dp):
            take(source)

    owner = (me == own_up) | (me == own_down) | (me == own_query) | (me == own_out)

    @pl.when(owner)
    def _():
        square = jnp.zeros((1, 1), jnp.float32)
        for start in range(0, total, width):
            part = columns(start)
            square = square + jnp.sum(part * part, keepdims=True)
        scale = 1.0 / (jnp.sqrt(square) + ORTHO_EPS)
        for start in range(0, total, width):
            part = columns(start) * scale
            wide[:, start : start + width] = part
            low[:, start : start + width] = part.astype(jnp.bfloat16)

        def turn(_, carry):
            gram = lax.dot_general(low[...], low[...], NT, preferred_element_type=jnp.float32)
            gram_low = gram.astype(jnp.bfloat16)
            twice = jnp.dot(gram_low, gram_low, preferred_element_type=jnp.float32)
            blend[...] = (NS_B * gram + NS_C * twice).astype(jnp.bfloat16)

            def piece(index, inner):
                where = pl.ds(pl.multiple_of(index * width, width), width)
                part = NS_A * wide[:, where] + jnp.dot(
                    blend[...], low[:, where], preferred_element_type=jnp.float32
                )
                wide[:, where] = part
                low[:, where] = part.astype(jnp.bfloat16)
                return inner

            return lax.fori_loop(0, total // width, piece, carry)

        lax.fori_loop(0, 5, turn, 0)
        if not turned:
            for start in range(0, total, width):
                held[start : start + width, :] = low[:, start : start + width].T

    result = low if turned else held

    def give(job, target, place):
        @pl.when(me != target)
        def _():
            pltpu.make_async_remote_copy(
                src_ref=slot(result, place), dst_ref=back.at[job],
                send_sem=return_sem.at[target], recv_sem=back_sem.at[job],
                device_id={"dp": target}, device_id_type=MESH,
            ).start()

        @pl.when(me == target)
        def _():
            back[job] = slot(result, place)[...]

    def gave(target):
        @pl.when(me != target)
        def _():
            pltpu.make_async_remote_copy(
                src_ref=slot(result, 0), dst_ref=back.at[0],
                send_sem=return_sem.at[target], recv_sem=back_sem.at[0],
                device_id={"dp": target}, device_id_type=MESH,
            ).wait_send()

    jobs = (
        (own_up, 0, 0, n_dp),
        (own_down, 1, 0, n_dp),
        (own_query, 2, 0, query_devices),
        (own_out, 2, query_devices, n_dp),
    )
    for who, job, first, last in jobs:
        @pl.when(me == who)
        def _():
            for target in range(first, last):
                give(job, target, target - first)
    rates = (LR_EXPERT, LR_EXPERT, jnp.where(me < query_devices, LR_QKV, LR_OUT))
    for job in (2, 0, 1):
        @pl.when(me != owners[job])
        def _():
            pltpu.make_async_remote_copy(
                src_ref=outgoing.at[job], dst_ref=back.at[job],
                send_sem=send_sem.at[job], recv_sem=back_sem.at[job],
                device_id={"dp": owners[job]}, device_id_type=MESH,
            ).wait()

        step = rates[job] * turn_over(back[job]).astype(jnp.float32)
        if job == 2:
            new = dense_master[...] - step
            dense_new[...] = new
            dense_copy[...] = new.astype(jnp.bfloat16)
        else:
            new = expert_master[0, job] - step
            expert_new[0, job] = new
            expert_copy[0, job] = new.astype(jnp.bfloat16)
    for who, job, first, last in jobs:
        @pl.when(me == who)
        def _():
            for target in range(first, last):
                gave(target)


def muon(expert_grad, dense_grad, expert_momentum, dense_momentum, expert_master, dense_master):
    n_dp = lax.axis_size("dp")
    rows, width = dense_grad.shape
    total = n_dp * rows
    block = (width, rows) if rows % 128 == 0 else (rows, width)
    whole = (width, total) if rows % 128 == 0 else (total, width)
    full = jax.ShapeDtypeStruct(expert_grad.shape, jnp.float32)
    flat = jax.ShapeDtypeStruct(dense_grad.shape, jnp.float32)
    vmem = pl.BlockSpec(memory_space=pltpu.VMEM)
    return pl.pallas_call(
        partial(muon_kernel, n_dp, width),
        out_shape=(
            full, flat, full, flat,
            jax.ShapeDtypeStruct(expert_grad.shape, jnp.bfloat16),
            jax.ShapeDtypeStruct(dense_grad.shape, jnp.bfloat16),
        ),
        in_specs=[vmem] * 6,
        out_specs=[vmem] * 6,
        scratch_shapes=[
            pltpu.VMEM((3, *block), jnp.bfloat16),
            pltpu.VMEM(whole, jnp.bfloat16),
            pltpu.VMEM((width, total), jnp.float32),
            pltpu.VMEM((width, total), jnp.bfloat16),
            pltpu.VMEM((width, width), jnp.bfloat16),
            pltpu.VMEM((3, *block), jnp.bfloat16),
            pltpu.SemaphoreType.DMA((3,)),
            pltpu.SemaphoreType.DMA((n_dp,)),
            pltpu.SemaphoreType.DMA((n_dp,)),
            pltpu.SemaphoreType.DMA((3,)),
        ],
        compiler_params=pltpu.CompilerParams(
            collective_id=1, has_side_effects=True, vmem_limit_bytes=48 * 1024 * 1024
        ),
        name="muon",
    )(expert_grad, dense_grad, expert_momentum, dense_momentum, expert_master, dense_master)


def shards(
    images,
    cotangent,
    gates,
    routes,
    slots,
    dense_master,
    dense_momentum,
    norm_master,
    norm_momentum,
    expert_master,
    expert_momentum,
):
    micro_count, images_here, seq, width = images.shape
    experts = lax.axis_size("expert")
    dp_count = lax.axis_size("dp")
    rows_dev = images_here * seq
    capacity = min(rows_dev, 4 * rows_dev // experts)
    slot_total = experts * capacity
    tokens_all = micro_count * rows_dev * dp_count * experts
    whole_experts = lax.all_gather(expert_master.astype(jnp.bfloat16), "dp", axis=2, tiled=True)
    w_up = whole_experts[0, 0]
    w_down = whole_experts[0, 1]
    dense_low = dense_master.astype(jnp.bfloat16)
    norm_low = norm_master.astype(jnp.bfloat16)
    grad_dense = jnp.zeros((4 * width, width), jnp.float32)
    grad_norm = jnp.zeros((4, width), jnp.float32)
    grad_up = jnp.zeros(w_up.shape, jnp.float32)
    grad_down = jnp.zeros(w_down.shape, jnp.float32)
    outputs_list = []
    input_list = []
    for micro in range(micro_count):
        dense_whole, norm_whole = (
            lax.all_gather(dense_low, "dp", axis=0, tiled=True),
            lax.all_gather(norm_low, "dp", axis=1, tiled=True),
        )
        norm_wide = norm_whole.astype(jnp.float32)
        block = images[micro].astype(jnp.float32).reshape(rows_dev, width)
        normed_full, normed_one, inverse_one = layer_norm(block, norm_wide[0], norm_wide[1])
        normed_one_low = normed_full.astype(jnp.bfloat16).reshape(images_here, seq, width)
        branch, kept = attention_forward(
            normed_one_low, dense_whole[: 3 * width], dense_whole[3 * width :], HEADS
        )
        residual = block + branch.reshape(rows_dev, width)
        normed_two_full, normed_two, inverse_two = layer_norm(residual, norm_wide[2], norm_wide[3])
        normed_two_low = normed_two_full.astype(jnp.bfloat16)
        index = (routes[micro] * capacity + slots[micro]).reshape(rows_dev, 2)
        gate_pair = gates[micro].reshape(rows_dev, 2)
        picks = jnp.arange(slot_total)[:, None, None] == index[None, :, :]
        dispatch = jnp.sum(picks.astype(jnp.int32), axis=2).astype(jnp.bfloat16)
        send = jnp.dot(dispatch, normed_two_low, preferred_element_type=jnp.float32).astype(
            jnp.bfloat16
        )
        received = lax.all_to_all(
            send.reshape(experts, capacity, width),
            "expert",
            split_axis=0,
            concat_axis=0,
            tiled=True,
        )
        sources, count, features = received.shape
        rows_in = received.reshape(sources * count, features)
        pre = jnp.einsum("rd,fd->rf", rows_in, w_up, preferred_element_type=jnp.float32)
        hidden = jax.nn.gelu(pre, approximate=False).astype(jnp.bfloat16)
        produced = jnp.dot(hidden, w_down, preferred_element_type=jnp.float32).astype(jnp.bfloat16)
        returned = lax.all_to_all(
            produced.reshape(sources, count, features),
            "expert",
            split_axis=0,
            concat_axis=0,
            tiled=True,
        )
        returned, received, pre = (returned, received, pre.reshape(sources, count, pre.shape[1]))
        back_flat = returned.reshape(slot_total, width)
        taken = back_flat[index].astype(jnp.float32)
        moe = gate_pair[:, 0:1] * taken[:, 0] + gate_pair[:, 1:2] * taken[:, 1]
        outputs_list.append((residual + moe).astype(jnp.bfloat16).reshape(images_here, seq, width))
        grad_output = cotangent[micro].astype(jnp.float32).reshape(rows_dev, width)
        spread = jnp.sum(jnp.where(picks, gate_pair[None, :, :], 0.0), axis=2)
        grad_send = jnp.dot(spread, grad_output, precision=HIGH).astype(jnp.bfloat16)
        grad_received = lax.all_to_all(
            grad_send.reshape(experts, capacity, width),
            "expert",
            split_axis=0,
            concat_axis=0,
            tiled=True,
        )
        grad_rows_out = grad_received.reshape(slot_total, width)
        pre_rows = pre.reshape(slot_total, pre.shape[2])
        hidden_full, gelu_pull = jax.vjp(partial(jax.nn.gelu, approximate=False), pre_rows)
        hidden = hidden_full.astype(jnp.bfloat16)
        grad_down = grad_down + jnp.einsum(
            "rf,rd->fd", hidden, grad_rows_out, preferred_element_type=jnp.float32
        )
        grad_hidden = jnp.einsum(
            "rd,fd->rf", grad_rows_out, w_down, preferred_element_type=jnp.float32
        )
        grad_pre = gelu_pull(grad_hidden)[0].astype(jnp.bfloat16)
        rows_in = received.reshape(slot_total, width)
        grad_up = grad_up + jnp.einsum(
            "rf,rd->fd", grad_pre, rows_in, preferred_element_type=jnp.float32
        )
        grad_in = jnp.dot(grad_pre, w_up, preferred_element_type=jnp.float32).astype(jnp.bfloat16)
        grad_back = lax.all_to_all(
            grad_in.reshape(experts, capacity, width),
            "expert",
            split_axis=0,
            concat_axis=0,
            tiled=True,
        )
        pair_back = grad_back.reshape(slot_total, width)[index].astype(jnp.float32)
        grad_normed_two = pair_back[:, 0] + pair_back[:, 1]
        grad_two_rows, gain_two_grad, bias_two_grad = norm_backward(
            grad_normed_two, normed_two, inverse_two, norm_wide[2]
        )
        grad_residual = grad_output + grad_two_rows
        dense_again, norm_again = (
            lax.all_gather(dense_low, "dp", axis=0, tiled=True),
            lax.all_gather(norm_low, "dp", axis=1, tiled=True),
        )
        norm_again_wide = norm_again.astype(jnp.float32)
        grad_normed_one, grad_qkv_w, grad_out_w = attention_backward(
            grad_residual.reshape(images_here, seq, width),
            normed_one_low,
            dense_again[: 3 * width],
            dense_again[3 * width :],
            kept,
            HEADS,
        )
        grad_one_rows, gain_one_grad, bias_one_grad = norm_backward(
            grad_normed_one.reshape(rows_dev, width), normed_one, inverse_one, norm_again_wide[0]
        )
        input_list.append(
            (grad_residual + grad_one_rows).astype(jnp.bfloat16).reshape(images_here, seq, width)
        )
        grad_dense = grad_dense + jnp.concatenate([grad_qkv_w, grad_out_w], axis=0)
        grad_norm = grad_norm + jnp.stack(
            [gain_one_grad, bias_one_grad, gain_two_grad, bias_two_grad]
        )
    expert_terms = jnp.stack([grad_up, grad_down])[None]
    summed_dense, summed_norm, expert_grad = (
        lax.psum_scatter(
            grad_dense.astype(jnp.bfloat16), "dp", scatter_dimension=0, tiled=True
        ).astype(jnp.float32),
        lax.psum_scatter(
            grad_norm.astype(jnp.bfloat16), "dp", scatter_dimension=1, tiled=True
        ).astype(jnp.float32),
        lax.psum_scatter(
            expert_terms.astype(jnp.bfloat16), "dp", scatter_dimension=2, tiled=True
        ).astype(jnp.float32),
    )
    dense_grad, norm_grad = (
        lax.psum(summed_dense.astype(jnp.bfloat16), "expert").astype(jnp.float32),
        lax.psum(summed_norm.astype(jnp.bfloat16), "expert").astype(jnp.float32),
    )
    norm_moment = DECAY * norm_momentum + norm_grad
    norm_new = norm_master - LR_VECTOR * tokens_all ** (-0.5) * norm_moment
    expert_moment, dense_moment, expert_new, dense_new, expert_copy, dense_copy = muon(
        expert_grad, dense_grad, expert_momentum, dense_momentum, expert_master, dense_master
    )
    return (
        jnp.stack(outputs_list),
        jnp.stack(input_list),
        dense_grad,
        norm_grad,
        expert_grad,
        dense_moment,
        norm_moment,
        expert_moment,
        dense_new,
        norm_new,
        expert_new,
        dense_copy,
        expert_copy,
    )


def solution(mesh):
    in_specs = (
        P(None, ("dp", "expert"), None, None),
        P(None, ("dp", "expert"), None, None),
        P(None, ("dp", "expert"), None, None),
        P(None, ("dp", "expert"), None, None),
        P(None, ("dp", "expert"), None, None),
        P("dp", None),
        P("dp", None),
        P(None, "dp"),
        P(None, "dp"),
        P("expert", None, "dp", None),
        P("expert", None, "dp", None),
    )
    out_specs = (
        P(None, ("dp", "expert"), None, None),
        P(None, ("dp", "expert"), None, None),
        P("dp", None),
        P(None, "dp"),
        P("expert", None, "dp", None),
        P("dp", None),
        P(None, "dp"),
        P("expert", None, "dp", None),
        P("dp", None),
        P(None, "dp"),
        P("expert", None, "dp", None),
        P("dp", None),
        P("expert", None, "dp", None),
    )
    return jax.shard_map(shards, mesh=mesh, in_specs=in_specs, out_specs=out_specs, check_vma=False)
```

```python
from functools import partial

import jax
import jax.numpy as jnp
from jax import lax
from jax.experimental import pallas as pl
from jax.experimental.pallas import tpu as pltpu
from jax.sharding import PartitionSpec as P

MESH = pl.DeviceIdType.MESH
NT = (((1,), (1,)), ((), ()))
TN = (((0,), (0,)), ((), ()))
ERF_P = 0.3275911 * 0.5**0.5
ERF_1 = 0.254829592
ERF_2 = -0.284496736
ERF_3 = 1.421413741
ERF_4 = -1.453152027
ERF_5 = 1.061405429
ROOT_TWO_PI = 0.3989422804014327

HEADS = 8


HIGH = lax.Precision.HIGHEST
NORM_EPS = 1e-06
ORTHO_EPS = 1e-07
NS_A = 3.4445
NS_B = -4.775
NS_C = 2.0315
DECAY = 0.5
LR_QKV = 0.5
LR_OUT = 1.5
LR_EXPERT = 0.5
LR_VECTOR = 0.05


def layer_norm(rows, norm_gain, norm_bias):
    row_mean = jnp.mean(rows, axis=-1, keepdims=True)
    centred = rows - row_mean
    variance = jnp.mean(centred * centred, axis=-1, keepdims=True)
    inverse = lax.rsqrt(variance + NORM_EPS)
    normed = centred * inverse
    return (normed * norm_gain + norm_bias, normed, inverse)


def norm_backward(grad_out, normed, inverse, norm_gain):
    grad_gain = jnp.sum(grad_out * normed, axis=0)
    grad_bias = jnp.sum(grad_out, axis=0)
    scaled = grad_out * norm_gain
    grad_rows = inverse * (
        scaled
        - jnp.mean(scaled, axis=-1, keepdims=True)
        - normed * jnp.mean(scaled * normed, axis=-1, keepdims=True)
    )
    return (grad_rows, grad_gain, grad_bias)


def split_heads(projected, heads):
    images_here, seq, triple = projected.shape
    head_size = triple // (3 * heads)
    parts = projected.reshape(images_here, seq, 3, heads, head_size)
    return (parts[:, :, 0], parts[:, :, 1], parts[:, :, 2], head_size ** (-0.5))


def attention_forward(normed_low, w_qkv, w_out, heads):
    images_here, seq, width = normed_low.shape
    projected = jnp.einsum(
        "bsd,ed->bse", normed_low, w_qkv, preferred_element_type=jnp.float32
    ).astype(jnp.bfloat16)
    query_part, key_part, value_part, score_scale = split_heads(projected, heads)
    scores = (
        jnp.einsum("bqhd,bkhd->bhqk", query_part, key_part, preferred_element_type=jnp.float32)
        * score_scale
    )
    top = jnp.max(scores, axis=-1, keepdims=True)
    expo = jnp.exp(scores - top)
    total = jnp.sum(expo, axis=-1, keepdims=True)
    soft_weights = expo / total
    log_total = top + jnp.log(total)
    mixed = jnp.einsum(
        "bhqk,bkhd->bqhd",
        soft_weights.astype(jnp.bfloat16),
        value_part,
        preferred_element_type=jnp.float32,
    )
    mixed = mixed.astype(jnp.bfloat16).reshape(images_here, seq, width)
    branch = jnp.einsum("bsd,ed->bse", mixed, w_out, preferred_element_type=jnp.float32)
    return (branch, (projected, log_total, mixed))


def attention_backward(grad_branch, normed_low, w_qkv, w_out, kept, heads):
    projected, log_total, mixed = kept
    images_here, seq, width = normed_low.shape
    query_part, key_part, value_part, score_scale = split_heads(projected, heads)
    grad_low = grad_branch.astype(jnp.bfloat16)
    grad_out_w = jnp.einsum("bse,bsd->ed", grad_low, mixed, preferred_element_type=jnp.float32)
    grad_mixed = jnp.einsum(
        "bse,ed->bsd", grad_low, w_out, preferred_element_type=jnp.float32
    ).astype(jnp.bfloat16)
    grad_mixed = grad_mixed.reshape(query_part.shape)
    scores = (
        jnp.einsum("bqhd,bkhd->bhqk", query_part, key_part, preferred_element_type=jnp.float32)
        * score_scale
    )
    soft_weights = jnp.exp(scores - log_total)
    soft_low = soft_weights.astype(jnp.bfloat16)
    grad_soft = jnp.einsum(
        "bqhd,bkhd->bhqk", grad_mixed, value_part, preferred_element_type=jnp.float32
    )
    grad_scores = (
        soft_weights * (grad_soft - jnp.sum(soft_weights * grad_soft, axis=-1, keepdims=True))
    ).astype(jnp.bfloat16)
    grad_query = (
        jnp.einsum("bhqk,bkhd->bqhd", grad_scores, key_part, preferred_element_type=jnp.float32)
        * score_scale
    )
    grad_key = (
        jnp.einsum("bhqk,bqhd->bkhd", grad_scores, query_part, preferred_element_type=jnp.float32)
        * score_scale
    )
    grad_value = jnp.einsum(
        "bhqk,bqhd->bkhd", soft_low, grad_mixed, preferred_element_type=jnp.float32
    )
    grad_projected = (
        jnp.stack([grad_query, grad_key, grad_value], axis=2)
        .reshape(images_here, seq, 3 * width)
        .astype(jnp.bfloat16)
    )
    grad_qkv_w = jnp.einsum(
        "bse,bsd->ed", grad_projected, normed_low, preferred_element_type=jnp.float32
    )
    grad_normed = jnp.einsum(
        "bse,ed->bsd", grad_projected, w_qkv, preferred_element_type=jnp.float32
    )
    return (grad_normed, grad_qkv_w, grad_out_w)


def muon_kernel(
    n_dp, width, expert_grad, dense_grad, expert_momentum, dense_momentum, expert_master,
    dense_master, expert_moment, dense_moment, expert_new, dense_new, expert_copy, dense_copy,
    outgoing, held, wide, low, blend, back, send_sem, take_sem, return_sem, back_sem,
):
    me = lax.axis_index("dp")
    rows = dense_grad.shape[0]
    turned = rows % 128 == 0

    def turn_over(block):
        return block.T if turned else block

    def slot(ref, place):
        where = pl.ds(pl.multiple_of(place * rows, rows), rows)
        return ref.at[:, where] if turned else ref.at[where, :]

    query_devices = 3 * width // rows
    own_up, own_down, own_query, own_out = 0, 3 * n_dp // 4, n_dp // 4, n_dp // 2
    dense_owner = jnp.where(me < query_devices, own_query, own_out)
    dense_place = jnp.where(me < query_devices, me, me - query_devices)
    barrier = pltpu.get_barrier_semaphore()
    for step in range(1, n_dp):
        pl.semaphore_signal(
            barrier, inc=1, device_id={"dp": lax.rem(me + step, n_dp)}, device_id_type=MESH
        )
    for job in range(2):
        moment = DECAY * expert_momentum[0, job] + expert_grad[0, job]
        expert_moment[0, job] = moment
        outgoing[job] = turn_over(moment.astype(jnp.bfloat16))
    moment = DECAY * dense_momentum[...] + dense_grad[...]
    dense_moment[...] = moment
    outgoing[2] = turn_over(moment.astype(jnp.bfloat16))
    pl.semaphore_wait(barrier, n_dp - 1)

    owners = (own_up, own_down, dense_owner)
    places = (me, me, dense_place)
    for job in range(3):
        @pl.when(me != owners[job])
        def _():
            pltpu.make_async_remote_copy(
                src_ref=outgoing.at[job], dst_ref=slot(held, places[job]),
                send_sem=send_sem.at[job], recv_sem=take_sem.at[me],
                device_id={"dp": owners[job]}, device_id_type=MESH,
            ).start()

        @pl.when(me == owners[job])
        def _():
            slot(held, places[job])[...] = outgoing[job]

    def take(source):
        @pl.when(me != source)
        def _():
            pltpu.make_async_remote_copy(
                src_ref=outgoing.at[0], dst_ref=slot(held, 0),
                send_sem=send_sem.at[0], recv_sem=take_sem.at[source],
                device_id={"dp": source}, device_id_type=MESH,
            ).wait_recv()

    query_rows = 3 * width
    out_rows = n_dp * rows - query_rows
    total = n_dp * rows

    def clear(first):
        zeros = jnp.zeros((total - first, width), jnp.bfloat16)
        if turned:
            held[:, first:] = zeros.T
        else:
            held[first:, :] = zeros

    def columns(start):
        where = slice(start, start + width)
        return (held[:, where] if turned else held[where, :].T).astype(jnp.float32)

    @pl.when((me == own_up) | (me == own_down))
    def _():
        for source in range(n_dp):
            take(source)

    @pl.when(me == own_query)
    def _():
        clear(query_rows)
        for source in range(query_devices):
            take(source)

    @pl.when(me == own_out)
    def _():
        clear(out_rows)
        for source in range(query_devices, n_dp):
            take(source)

    owner = (me == own_up) | (me == own_down) | (me == own_query) | (me == own_out)

    @pl.when(owner)
    def _():
        square = jnp.zeros((1, 1), jnp.float32)
        for start in range(0, total, width):
            part = columns(start)
            square = square + jnp.sum(part * part, keepdims=True)
        scale = 1.0 / (jnp.sqrt(square) + ORTHO_EPS)
        for start in range(0, total, width):
            part = columns(start) * scale
            wide[:, start : start + width] = part
            low[:, start : start + width] = part.astype(jnp.bfloat16)

        def turn(_, carry):
            gram = lax.dot_general(low[...], low[...], NT, preferred_element_type=jnp.float32)
            gram_low = gram.astype(jnp.bfloat16)
            twice = jnp.dot(gram_low, gram_low, preferred_element_type=jnp.float32)
            blend[...] = (NS_B * gram + NS_C * twice).astype(jnp.bfloat16)

            def piece(index, inner):
                where = pl.ds(pl.multiple_of(index * width, width), width)
                part = NS_A * wide[:, where] + jnp.dot(
                    blend[...], low[:, where], preferred_element_type=jnp.float32
                )
                wide[:, where] = part
                low[:, where] = part.astype(jnp.bfloat16)
                return inner

            return lax.fori_loop(0, total // width, piece, carry)

        lax.fori_loop(0, 5, turn, 0)
        if not turned:
            for start in range(0, total, width):
                held[start : start + width, :] = low[:, start : start + width].T

    result = low if turned else held

    def give(job, target, place):
        @pl.when(me != target)
        def _():
            pltpu.make_async_remote_copy(
                src_ref=slot(result, place), dst_ref=back.at[job],
                send_sem=return_sem.at[target], recv_sem=back_sem.at[job],
                device_id={"dp": target}, device_id_type=MESH,
            ).start()

        @pl.when(me == target)
        def _():
            back[job] = slot(result, place)[...]

    def gave(target):
        @pl.when(me != target)
        def _():
            pltpu.make_async_remote_copy(
                src_ref=slot(result, 0), dst_ref=back.at[0],
                send_sem=return_sem.at[target], recv_sem=back_sem.at[0],
                device_id={"dp": target}, device_id_type=MESH,
            ).wait_send()

    jobs = (
        (own_up, 0, 0, n_dp),
        (own_down, 1, 0, n_dp),
        (own_query, 2, 0, query_devices),
        (own_out, 2, query_devices, n_dp),
    )
    for who, job, first, last in jobs:
        @pl.when(me == who)
        def _():
            for target in range(first, last):
                give(job, target, target - first)
    rates = (LR_EXPERT, LR_EXPERT, jnp.where(me < query_devices, LR_QKV, LR_OUT))
    for job in (2, 0, 1):
        @pl.when(me != owners[job])
        def _():
            pltpu.make_async_remote_copy(
                src_ref=outgoing.at[job], dst_ref=back.at[job],
                send_sem=send_sem.at[job], recv_sem=back_sem.at[job],
                device_id={"dp": owners[job]}, device_id_type=MESH,
            ).wait()

        step = rates[job] * turn_over(back[job]).astype(jnp.float32)
        if job == 2:
            new = dense_master[...] - step
            dense_new[...] = new
            dense_copy[...] = new.astype(jnp.bfloat16)
        else:
            new = expert_master[0, job] - step
            expert_new[0, job] = new
            expert_copy[0, job] = new.astype(jnp.bfloat16)
    for who, job, first, last in jobs:
        @pl.when(me == who)
        def _():
            for target in range(first, last):
                gave(target)


def muon(expert_grad, dense_grad, expert_momentum, dense_momentum, expert_master, dense_master):
    n_dp = lax.axis_size("dp")
    rows, width = dense_grad.shape
    total = n_dp * rows
    block = (width, rows) if rows % 128 == 0 else (rows, width)
    whole = (width, total) if rows % 128 == 0 else (total, width)
    full = jax.ShapeDtypeStruct(expert_grad.shape, jnp.float32)
    flat = jax.ShapeDtypeStruct(dense_grad.shape, jnp.float32)
    vmem = pl.BlockSpec(memory_space=pltpu.VMEM)
    return pl.pallas_call(
        partial(muon_kernel, n_dp, width),
        out_shape=(
            full, flat, full, flat,
            jax.ShapeDtypeStruct(expert_grad.shape, jnp.bfloat16),
            jax.ShapeDtypeStruct(dense_grad.shape, jnp.bfloat16),
        ),
        in_specs=[vmem] * 6,
        out_specs=[vmem] * 6,
        scratch_shapes=[
            pltpu.VMEM((3, *block), jnp.bfloat16),
            pltpu.VMEM(whole, jnp.bfloat16),
            pltpu.VMEM((width, total), jnp.float32),
            pltpu.VMEM((width, total), jnp.bfloat16),
            pltpu.VMEM((width, width), jnp.bfloat16),
            pltpu.VMEM((3, *block), jnp.bfloat16),
            pltpu.SemaphoreType.DMA((3,)),
            pltpu.SemaphoreType.DMA((n_dp,)),
            pltpu.SemaphoreType.DMA((n_dp,)),
            pltpu.SemaphoreType.DMA((3,)),
        ],
        compiler_params=pltpu.CompilerParams(
            collective_id=1, has_side_effects=True, vmem_limit_bytes=48 * 1024 * 1024
        ),
        name="muon",
    )(expert_grad, dense_grad, expert_momentum, dense_momentum, expert_master, dense_master)


def nn(a, b):
    return jnp.dot(a, b, preferred_element_type=jnp.float32)


def nt(a, b):
    return lax.dot_general(a, b, NT, preferred_element_type=jnp.float32)


def tn(a, b):
    return lax.dot_general(a, b, TN, preferred_element_type=jnp.float32)


def gelu_parts(pre):
    bell = jnp.exp(-0.5 * pre * pre)
    share = 1.0 / (1.0 + ERF_P * jnp.abs(pre))
    series = share * (ERF_1 + share * (ERF_2 + share * (ERF_3 + share * (ERF_4 + share * ERF_5))))
    tail = 0.5 * series * bell
    return jnp.where(pre >= 0.0, 1.0 - tail, tail), bell * ROOT_TWO_PI


def row_stats(rows):
    mean = jnp.mean(rows, axis=-1, keepdims=True)
    centred = rows - mean
    inverse = lax.rsqrt(jnp.mean(centred * centred, axis=-1, keepdims=True) + NORM_EPS)
    return centred * inverse, inverse


def rows_backward(grad_out, normed, inverse, gain):
    scaled = grad_out * gain
    return inverse * (
        scaled
        - jnp.mean(scaled, axis=-1, keepdims=True)
        - normed * jnp.mean(scaled * normed, axis=-1, keepdims=True)
    )


def block_kernel(
    cfg, images, cotangent, weights, dense_master, norm_master, expert_master,
    activations, input_grad, dense_grad, norm_grad, expert_grad,
    dense, experts, norm_slots, norms, tokens, outer_low, normed_low, projected, soft, mixed, residual,
    rows_x, rows_dy, turned_x, turned_dy, weight_slots, hidden_low, grad_pre_low,
    produced_sum, grad_in_sum, produced_out, grad_in_out, produced_got, grad_in_got,
    expert_sum, pair_out, pair_got, chip_got, grad_projected, grad_branch,
    dense_sum, dense_out, dense_got, dense_chip, line_out, line_got, line_all, norm_all, norm_line,
    dense_send, dense_take, expert_send, expert_take, norm_send, norm_take,
    dy_send, dy_take, weight_send, weight_take, x_send, x_take, g_send, g_take, p_send, p_take,
    pair_send, pair_take, chip_send, chip_take, dpair_send, dpair_take, dchip_send, dchip_take,
    line_send, line_take, lall_send, lall_take, nall_send, nall_take, nline_send, nline_take,
):
    n_dp, n_ex, micro_count, seq, pad, width, heads = cfg
    me, spot = lax.axis_index("dp"), lax.axis_index("expert")
    core = lax.rem(me, 2)
    partner = me + 1 - 2 * core
    chips = n_dp // 2
    chip = me // 2
    bf16 = jnp.bfloat16
    shard = expert_master.shape[2]
    dense_shard = dense_master.shape[0]
    norm_shard = norm_master.shape[1]
    line_rows = n_ex * pad
    head_size = width // heads
    score_scale = head_size ** (-0.5)

    def copy(src, dst, send, take, device):
        return pltpu.make_async_remote_copy(
            src_ref=src, dst_ref=dst, send_sem=send, recv_sem=take,
            device_id=device, device_id_type=MESH,
        )

    def over_dp(step):
        return lax.rem(me + step, n_dp)

    def over_ex(step):
        return lax.rem(spot + step, n_ex)

    def at_row(ref, index, size):
        return ref.at[pl.ds(pl.multiple_of(index * size, size), size)]

    barrier = pltpu.get_barrier_semaphore()
    for step in range(1, n_dp):
        pl.semaphore_signal(barrier, inc=1, device_id={"dp": over_dp(step)}, device_id_type=MESH)
    for step in range(1, n_ex):
        pl.semaphore_signal(barrier, inc=1, device_id={"expert": over_ex(step)}, device_id_type=MESH)

    at_row(dense, me, dense_shard)[...] = dense_master[...].astype(bf16)
    for job in range(2):
        at_row(experts.at[job], me, shard)[...] = expert_master[0, job].astype(bf16)
    norm_slots[me] = jnp.zeros(norm_slots.shape[1:], jnp.float32)
    norm_slots[me, 0:4, 0:norm_shard] = norm_master[...].astype(bf16).astype(jnp.float32)
    weight_slots[spot] = weights[...]
    tail = seq // 16 * 16
    for micro in range(micro_count):
        tokens[micro, tail:] = jnp.zeros((pad - tail, width), bf16)
        tokens[micro, 0:seq] = images[micro]
        outer_low[micro, tail:] = jnp.zeros((pad - tail, width), bf16)
        outer_low[micro, 0:seq] = cotangent[micro]
        rows_dy[micro, pl.ds(pl.multiple_of(spot * pad, 16), pad)] = outer_low[micro]
        rows_x[micro, line_rows:] = jnp.zeros((rows_x.shape[1] - line_rows, width), bf16)
        rows_dy[micro, line_rows:] = jnp.zeros((rows_x.shape[1] - line_rows, width), bf16)
    hidden_low[line_rows:] = jnp.zeros((rows_x.shape[1] - line_rows, shard), bf16)
    grad_pre_low[line_rows:] = jnp.zeros((rows_x.shape[1] - line_rows, shard), bf16)
    pl.semaphore_wait(barrier, n_dp + n_ex - 2)

    def gather_copy(views, source, target, send, take):
        return [copy(view(source), view(source), send.at[k], take.at[k], {"dp": target}) for k, view in enumerate(views)]

    def gather_start(views, send, take):
        for step in range(0, n_dp, 2):
            target = over_dp(step) if step else partner
            for k, view in enumerate(views):
                copy(view(me), view(me), send.at[k, step], take.at[k, me], {"dp": target}).start()

    def gather_pass(views, send, take):
        for step in range(2, n_dp, 2):
            source = lax.rem(me + n_dp - step, n_dp)
            for k, view in enumerate(views):
                copy(view(source), view(source), send.at[k, step], take.at[k, source], {"dp": partner}).wait_recv()
                copy(view(source), view(source), send.at[k, step + 1], take.at[k, source], {"dp": partner}).start()

    def gather_end(views, send, take):
        for step in range(0, n_dp, 2):
            source = lax.rem(partner + n_dp - step, n_dp)
            for k, view in enumerate(views):
                copy(view(source), view(source), send.at[k, step], take.at[k, source], {"dp": partner}).wait_recv()
        for step in range(n_dp):
            if step != 1:
                for k, view in enumerate(views):
                    copy(view(me), view(me), send.at[k, step], take.at[k, me], {"dp": partner}).wait_send()

    dense_views = [lambda i: at_row(dense, i, dense_shard)]
    expert_views = [lambda i, job=job: at_row(experts.at[job], i, shard) for job in range(2)]
    for step in range(1, n_dp):
        copy(norm_slots.at[me], norm_slots.at[me], norm_send.at[step], norm_take.at[me], {"dp": over_dp(step)}).start()
    gather_start(dense_views, dense_send, dense_take)

    def line(ref, micro, index):
        return ref.at[micro, pl.ds(pl.multiple_of(index * pad, 16), pad)]

    def spread(ref, micro, send, take):
        for step in range(1, n_ex):
            copy(line(ref, micro, spot), line(ref, micro, spot), send.at[micro, step], take.at[micro, spot], {"expert": over_ex(step)}).start()

    def spread_end(ref, micro, send, take):
        for step in range(1, n_ex):
            source = over_ex(step)
            copy(line(ref, micro, source), line(ref, micro, source), send.at[micro, step], take.at[micro, source], {"expert": source}).wait()

    for step in range(1, n_ex):
        copy(weight_slots.at[spot], weight_slots.at[spot], weight_send.at[step], weight_take.at[spot], {"expert": over_ex(step)}).start()
    spread(rows_dy, 0, dy_send, dy_take)

    for step in range(1, n_dp):
        source = over_dp(step)
        copy(norm_slots.at[source], norm_slots.at[source], norm_send.at[step], norm_take.at[source], {"dp": source}).wait()
    lane = lax.broadcasted_iota(jnp.int32, (128, width), 0)
    column = lax.broadcasted_iota(jnp.int32, (128, width), 1)
    wide = jnp.zeros((8, width), jnp.float32)
    for index in range(n_dp):
        pick = ((column - norm_shard * index == lane) & (lane < norm_shard)).astype(jnp.float32).astype(bf16)
        wide = wide + nn(norm_slots[index].astype(bf16), pick)
    norms[...] = wide

    gather_pass(dense_views, dense_send, dense_take)
    gather_start(expert_views, expert_send, expert_take)
    gather_end(dense_views, dense_send, dense_take)

    half = lax.broadcasted_iota(jnp.int32, (pad, 128), 1) < head_size
    low_masks = [half.astype(jnp.float32).astype(bf16), (1.0 - half.astype(jnp.float32)).astype(bf16)]
    real_key = lax.broadcasted_iota(jnp.int32, (pad, pad), 1) < seq

    def pair_of(micro, part, index):
        first = part * width + index * 128
        return projected[micro, :, first : first + 128]

    def attend(micro, carry):
        normed, _ = row_stats(tokens[micro].astype(jnp.float32))
        low = (normed * norms[0:1] + norms[1:2]).astype(bf16)
        normed_low[micro] = low
        projected[micro] = nt(low, dense[0 : 3 * width]).astype(bf16)
        for index in range(heads // 2):
            query, key, value = (pair_of(micro, part, index) for part in range(3))
            parts = []
            for side in range(2):
                scores = nt(query * low_masks[side], key) * score_scale
                scores = jnp.where(real_key, scores, -1e30)
                top = jnp.max(scores, axis=-1, keepdims=True)
                expo = jnp.exp(scores - top)
                weight = expo / jnp.sum(expo, axis=-1, keepdims=True)
                soft[micro, 2 * index + side] = weight
                parts.append(nn(weight.astype(bf16), value))
            mixed[micro, :, index * 128 : (index + 1) * 128] = jnp.where(half, parts[0], parts[1]).astype(bf16)
        total = tokens[micro].astype(jnp.float32) + nt(mixed[micro], dense[3 * width :])
        residual[micro] = total
        normed, _ = row_stats(total)
        line(rows_x, micro, spot)[...] = (normed * norms[2:3] + norms[3:4]).astype(bf16)
        spread(rows_x, micro, x_send, x_take)
        return carry

    lax.fori_loop(0, micro_count, attend, 0)
    for micro in range(1, micro_count):
        spread(rows_dy, micro, dy_send, dy_take)
    for step in range(1, n_ex):
        source = over_ex(step)
        copy(weight_slots.at[source], weight_slots.at[source], weight_send.at[step], weight_take.at[source], {"expert": source}).wait()
    gather_pass(expert_views, expert_send, expert_take)
    gather_end(expert_views, expert_send, expert_take)

    def column_of(slot, micro, row):
        picked = jnp.broadcast_to(weight_slots[slot, micro, pl.ds(row, 1)], (8, weight_slots.shape[3]))
        return picked.T[0:pad, 0:1]

    def send_back(out, got, micro, send, take):
        for step in range(1, n_ex):
            target = over_ex(step)
            copy(line(out, micro, target), line(got, micro, spot), send.at[micro, step], take.at[micro, spot], {"expert": target}).start()

    def send_back_end(out, got, micro, send, take):
        for step in range(1, n_ex):
            source = over_ex(step)
            copy(line(out, micro, source), line(got, micro, source), send.at[micro, step], take.at[micro, source], {"expert": source}).wait()

    for micro in range(micro_count):
        spread_end(rows_dy, micro, dy_send, dy_take)
        spread_end(rows_x, micro, x_send, x_take)
        for block in range(n_ex):
            where = slice(block * pad, (block + 1) * pad)
            rows_dy[micro, where] = (column_of(block, micro, spot) * rows_dy[micro, where].astype(jnp.float32)).astype(bf16)
        turned_x[...] = rows_x[micro].T
        turned_dy[...] = rows_dy[micro].T
        produced_sum[...] = jnp.zeros(produced_sum.shape, jnp.float32)
        grad_in_sum[...] = jnp.zeros(grad_in_sum.shape, jnp.float32)
        last = micro == micro_count - 1

        def chunk(count, carry, micro=micro, last=last):
            place = lax.rem(chip + 1 + count // 2, chips)
            index = 2 * place + lax.rem(count, 2)
            up = at_row(experts.at[0], index, shard)[...]
            down = at_row(experts.at[1], index, shard)[...]
            pre = nt(rows_x[micro, 0:line_rows], up)
            below, density = gelu_parts(pre)
            hidden_low[0:line_rows] = (pre * below).astype(bf16)
            produced_sum[...] += nn(hidden_low[0:line_rows], down)
            slope = below + pre * density
            grad_pre_low[0:line_rows] = (nt(rows_dy[micro, 0:line_rows], down) * slope).astype(bf16)
            grad_in_sum[...] += nn(grad_pre_low[0:line_rows], up)
            up_grad = nn(turned_x[...], grad_pre_low[...])
            down_grad = nn(turned_dy[...], hidden_low[...])
            if micro > 0:
                up_grad = up_grad + expert_sum[index, 0]
                down_grad = down_grad + expert_sum[index, 1]
            expert_sum[index, 0] = up_grad
            expert_sum[index, 1] = down_grad
            if last:
                @pl.when(lax.rem(count, 2) != core)
                def _():
                    pair_out[place] = expert_sum[index].astype(bf16)
                    copy(pair_out.at[place], pair_got.at[place], pair_send.at[place], pair_take.at[place], {"dp": partner}).start()

                @pl.when((lax.rem(count, 2) == 1) & (count >= 3))
                def _():
                    chip_step(lax.rem(chip + count // 2, chips))
            return carry

        def chip_step(place):
            index = 2 * place + core
            copy(pair_out.at[place], pair_got.at[place], pair_send.at[place], pair_take.at[place], {"dp": partner}).wait()
            for job in range(2):
                pair_got[place, job] = (expert_sum[index, job] + pair_got[place, job].astype(jnp.float32)).astype(bf16)
            copy(pair_got.at[place], chip_got.at[chip], chip_send.at[place], chip_take.at[chip], {"dp": index}).start()

        lax.fori_loop(0, n_dp, chunk, 0)
        grad_in_out[micro] = grad_in_sum[...].astype(bf16)
        send_back(grad_in_out, grad_in_got, micro, g_send, g_take)
        produced_out[micro] = produced_sum[...].astype(bf16)

    def combine(out, got, micro):
        line(got, micro, spot)[...] = line(out, micro, spot)[...]

    def attend_back(micro, carry):
        send_back_end(grad_in_out, grad_in_got, micro, g_send, g_take)
        combine(grad_in_out, grad_in_got, micro)
        incoming = jnp.zeros((pad, width), jnp.float32)
        for index in range(n_ex):
            incoming = incoming + grad_in_got[micro, index * pad : (index + 1) * pad].astype(jnp.float32)
        normed, inverse = row_stats(residual[micro])
        gain_two = jnp.sum(incoming * normed, axis=0, keepdims=True)
        bias_two = jnp.sum(incoming, axis=0, keepdims=True)
        total = outer_low[micro].astype(jnp.float32) + rows_backward(incoming, normed, inverse, norms[2:3])
        branch_low = total.astype(bf16)
        grad_branch[pl.ds(pl.multiple_of(micro * pad, 16), pad)] = branch_low
        grad_mixed = nn(branch_low, dense[3 * width :]).astype(bf16)
        for index in range(heads // 2):
            query, key, value = (pair_of(micro, part, index) for part in range(3))
            grad_pair = grad_mixed[:, index * 128 : (index + 1) * 128]
            parts = []
            for side in range(2):
                weight = soft[micro, 2 * index + side]
                grad_soft = nt(grad_pair * low_masks[side], value)
                grad_scores = (
                    weight * (grad_soft - jnp.sum(weight * grad_soft, axis=-1, keepdims=True))
                ).astype(bf16)
                parts.append((
                    nn(grad_scores, key) * score_scale,
                    tn(grad_scores, query) * score_scale,
                    tn(weight.astype(bf16), grad_pair),
                ))
            for part in range(3):
                first = part * width + index * 128
                grad_projected[pl.ds(pl.multiple_of(micro * pad, 16), pad), first : first + 128] = jnp.where(
                    half, parts[0][part], parts[1][part]
                ).astype(bf16)
        back = nn(grad_projected[pl.ds(pl.multiple_of(micro * pad, 16), pad)], dense[0 : 3 * width])
        normed, inverse = row_stats(tokens[micro].astype(jnp.float32))
        gain_one = jnp.sum(back * normed, axis=0, keepdims=True)
        bias_one = jnp.sum(back, axis=0, keepdims=True)
        total = total + rows_backward(back, normed, inverse, norms[0:1])
        input_grad[micro] = total[0:seq].astype(bf16)
        for row, part in enumerate((gain_one, bias_one, gain_two, bias_two)):
            norm_all[me, row : row + 1] += part
        return carry

    norm_all[me] = jnp.zeros((8, width), jnp.float32)
    depth = grad_branch.shape[0]
    if depth > micro_count * pad:
        grad_projected[micro_count * pad :] = jnp.zeros((depth - micro_count * pad, 3 * width), bf16)
        grad_branch[micro_count * pad :] = jnp.zeros((depth - micro_count * pad, width), bf16)
    lax.fori_loop(0, micro_count, attend_back, 0)

    for micro in range(micro_count):
        send_back(produced_out, produced_got, micro, p_send, p_take)
    for step in range(1, n_dp):
        copy(norm_all.at[me], norm_all.at[me], nall_send.at[step], nall_take.at[me], {"dp": over_dp(step)}).start()

    depth = grad_branch.shape[0]
    spare = [jnp.zeros((depth - micro_count * pad, width), bf16)] if depth > micro_count * pad else []
    turned_x[:, 0:depth] = jnp.concatenate([normed_low[micro] for micro in range(micro_count)] + spare, axis=0).T
    turned_dy[:, 0:depth] = jnp.concatenate([mixed[micro] for micro in range(micro_count)] + spare, axis=0).T

    def dense_chunk(count, carry):
        place = lax.rem(chip + 1 + count // 2, chips)
        index = 2 * place + lax.rem(count, 2)
        in_query = index * dense_shard < 3 * width

        @pl.when(in_query)
        def _():
            dense_sum[chips] = nn(turned_x[:, 0:depth], grad_projected[:, pl.ds(pl.multiple_of(jnp.where(in_query, index, 0) * dense_shard, 128), dense_shard)])

        @pl.when(jnp.logical_not(in_query))
        def _():
            first = jnp.where(in_query, 0, index * dense_shard - 3 * width)
            dense_sum[chips] = nn(turned_dy[:, 0:depth], grad_branch[:, pl.ds(pl.multiple_of(first, 128), dense_shard)])

        @pl.when(lax.rem(count, 2) == core)
        def _():
            dense_sum[place] = dense_sum[chips]

        @pl.when(lax.rem(count, 2) != core)
        def _():
            dense_out[place] = dense_sum[chips].astype(bf16)
            copy(dense_out.at[place], dense_got.at[place], dpair_send.at[place], dpair_take.at[place], {"dp": partner}).start()

        @pl.when((lax.rem(count, 2) == 1) & (count >= 3))
        def _():
            before = lax.rem(chip + count // 2, chips)
            copy(dense_out.at[before], dense_got.at[before], dpair_send.at[before], dpair_take.at[before], {"dp": partner}).wait()
            dense_got[before] = (dense_sum[before] + dense_got[before].astype(jnp.float32)).astype(bf16)
            copy(dense_got.at[before], dense_chip.at[chip], dchip_send.at[before], dchip_take.at[chip], {"dp": 2 * before + core}).start()
        return carry

    lax.fori_loop(0, n_dp, dense_chunk, 0)

    copy(pair_out.at[chip], pair_got.at[chip], pair_send.at[chip], pair_take.at[chip], {"dp": partner}).wait()
    for job in range(2):
        expert_sum[me, job] = expert_sum[me, job] + pair_got[chip, job].astype(jnp.float32)
    for step in range(1, chips):
        place = lax.rem(chip + step, chips)
        copy(pair_got.at[place], chip_got.at[place], chip_send.at[place], chip_take.at[place], {"dp": 2 * place + core}).wait()
        for job in range(2):
            expert_sum[me, job] = expert_sum[me, job] + chip_got[place, job].astype(jnp.float32)
    for job in range(2):
        expert_grad[0, job] = expert_sum[me, job].T

    copy(dense_out.at[chip], dense_got.at[chip], dpair_send.at[chip], dpair_take.at[chip], {"dp": partner}).wait()
    plane = dense_sum[chip] + dense_got[chip].astype(jnp.float32)
    for step in range(1, chips):
        place = lax.rem(chip + step, chips)
        copy(dense_got.at[place], dense_chip.at[place], dchip_send.at[place], dchip_take.at[place], {"dp": 2 * place + core}).wait()
        plane = plane + dense_chip[place].astype(jnp.float32)
    quarter = width // n_ex
    for index in range(n_ex):
        line_out[index] = plane[index * quarter : (index + 1) * quarter].astype(bf16)
    for step in range(1, n_ex):
        target = over_ex(step)
        copy(line_out.at[target], line_got.at[spot], line_send.at[step], line_take.at[spot], {"expert": target}).start()
    for step in range(1, n_dp):
        source = over_dp(step)
        copy(norm_all.at[source], norm_all.at[source], nall_send.at[step], nall_take.at[source], {"dp": source}).wait()
    norm_total = norm_all[0]
    for index in range(1, n_dp):
        norm_total = norm_total + norm_all[index]
    norm_line[spot] = norm_total
    for step in range(1, n_ex):
        copy(norm_line.at[spot], norm_line.at[spot], nline_send.at[step], nline_take.at[spot], {"expert": over_ex(step)}).start()
    summed = line_out[spot].astype(jnp.float32)
    for step in range(1, n_ex):
        source = over_ex(step)
        copy(line_out.at[source], line_got.at[source], line_send.at[step], line_take.at[source], {"expert": source}).wait()
        summed = summed + line_got[source].astype(jnp.float32)
    line_all[spot] = summed.astype(bf16)
    for step in range(1, n_ex):
        copy(line_all.at[spot], line_all.at[spot], lall_send.at[step], lall_take.at[spot], {"expert": over_ex(step)}).start()

    for micro in range(micro_count):
        send_back_end(produced_out, produced_got, micro, p_send, p_take)
        combine(produced_out, produced_got, micro)
        total = residual[micro]
        for index in range(n_ex):
            gate = weight_slots[spot, micro].T[0:pad, index : index + 1]
            total = total + gate * produced_got[micro, index * pad : (index + 1) * pad].astype(jnp.float32)
        activations[micro] = total[0:seq].astype(bf16)

    for step in range(1, n_ex):
        source = over_ex(step)
        copy(norm_line.at[source], norm_line.at[source], nline_send.at[step], nline_take.at[source], {"expert": source}).wait()
        copy(line_all.at[source], line_all.at[source], lall_send.at[step], lall_take.at[source], {"expert": source}).wait()
    norm_total = norm_line[0]
    for index in range(1, n_ex):
        norm_total = norm_total + norm_line[index]
    for index in range(n_dp):
        @pl.when(me == index)
        def _():
            norm_grad[...] = norm_total[0:4, index * norm_shard : (index + 1) * norm_shard]
    for index in range(n_ex):
        dense_grad[:, index * quarter : (index + 1) * quarter] = line_all[index].astype(jnp.float32).T


def block(images, cotangent, gates, routes, dense_master, norm_master, expert_master):
    micro_count, _, seq, width = images.shape
    n_dp, n_ex = lax.axis_size("dp"), lax.axis_size("expert")
    pad = -(-seq // 16) * 16
    lanes = -(-seq // 128) * 128
    shard, dense_shard, norm_shard = expert_master.shape[2], dense_master.shape[0], norm_master.shape[1]
    chips = n_dp // 2
    line_rows = n_ex * pad
    line_pad = -(-line_rows // 128) * 128
    slots = -(-n_ex // 8) * 8
    depth = -(-micro_count * pad // 128) * 128
    named = routes[:, 0, None, :, :] == jnp.arange(slots)[None, :, None, None]
    weights = jnp.sum(jnp.where(named, gates[:, 0, None, :, :], 0.0), axis=3)
    weights = jnp.pad(weights, ((0, 0), (0, 0), (0, lanes - seq)))
    vmem = pl.BlockSpec(memory_space=pltpu.VMEM)
    bf16, f32 = jnp.bfloat16, jnp.float32
    dma = pltpu.SemaphoreType.DMA
    tokens = (micro_count, pad, width)
    scratch = [
        pltpu.VMEM((n_dp * dense_shard, width), bf16),
        pltpu.VMEM((2, n_dp * shard, width), bf16),
        pltpu.VMEM((n_dp, 8, 128), f32),
        pltpu.VMEM((8, width), f32),
        pltpu.VMEM(tokens, bf16),
        pltpu.VMEM(tokens, bf16),
        pltpu.VMEM(tokens, bf16),
        pltpu.VMEM((micro_count, pad, 3 * width), bf16),
        pltpu.VMEM((micro_count, HEADS, pad, pad), f32),
        pltpu.VMEM(tokens, bf16),
        pltpu.VMEM(tokens, f32),
        pltpu.VMEM((micro_count, line_pad, width), bf16),
        pltpu.VMEM((micro_count, line_pad, width), bf16),
        pltpu.VMEM((width, line_pad), bf16),
        pltpu.VMEM((width, line_pad), bf16),
        pltpu.VMEM((n_ex, micro_count, slots, lanes), f32),
        pltpu.VMEM((line_pad, shard), bf16),
        pltpu.VMEM((line_pad, shard), bf16),
        pltpu.VMEM((line_rows, width), f32),
        pltpu.VMEM((line_rows, width), f32),
        pltpu.VMEM((micro_count, line_rows, width), bf16),
        pltpu.VMEM((micro_count, line_rows, width), bf16),
        pltpu.VMEM((micro_count, line_rows, width), bf16),
        pltpu.VMEM((micro_count, line_rows, width), bf16),
        pltpu.VMEM((n_dp, 2, width, shard), f32),
        pltpu.VMEM((chips, 2, width, shard), bf16),
        pltpu.VMEM((chips, 2, width, shard), bf16),
        pltpu.VMEM((chips, 2, width, shard), bf16),
        pltpu.VMEM((depth, 3 * width), bf16),
        pltpu.VMEM((depth, width), bf16),
        pltpu.VMEM((chips + 1, width, dense_shard), f32),
        pltpu.VMEM((chips, width, dense_shard), bf16),
        pltpu.VMEM((chips, width, dense_shard), bf16),
        pltpu.VMEM((chips, width, dense_shard), bf16),
        pltpu.VMEM((n_ex, width // n_ex, dense_shard), bf16),
        pltpu.VMEM((n_ex, width // n_ex, dense_shard), bf16),
        pltpu.VMEM((n_ex, width // n_ex, dense_shard), bf16),
        pltpu.VMEM((n_dp, 8, width), f32),
        pltpu.VMEM((n_ex, 8, width), f32),
    ]
    sems = [(1, n_dp), (1, n_dp), (2, n_dp), (2, n_dp), (n_dp,), (n_dp,)]
    sems += [(micro_count, n_ex)] * 2 + [(n_ex,)] * 2 + [(micro_count, n_ex)] * 6
    sems += [(chips,)] * 8 + [(n_ex,)] * 4 + [(n_dp,)] * 2 + [(n_ex,)] * 2
    cfg = (n_dp, n_ex, micro_count, seq, pad, width, HEADS)
    return pl.pallas_call(
        partial(block_kernel, cfg),
        out_shape=(
            jax.ShapeDtypeStruct((micro_count, seq, width), bf16),
            jax.ShapeDtypeStruct((micro_count, seq, width), bf16),
            jax.ShapeDtypeStruct(dense_master.shape, f32),
            jax.ShapeDtypeStruct(norm_master.shape, f32),
            jax.ShapeDtypeStruct(expert_master.shape, f32),
        ),
        in_specs=[vmem] * 6,
        out_specs=[vmem] * 5,
        scratch_shapes=scratch + [dma(shape) for shape in sems],
        compiler_params=pltpu.CompilerParams(
            collective_id=2, has_side_effects=True, vmem_limit_bytes=67043328
        ),
        name="block",
    )(images[:, 0], cotangent[:, 0], weights, dense_master, norm_master, expert_master)


def block_plain(images, cotangent, gates, routes, slots, dense_master, norm_master, expert_master):
    micro_count, images_here, seq, width = images.shape
    experts = lax.axis_size("expert")
    dp_count = lax.axis_size("dp")
    rows_dev = images_here * seq
    capacity = min(rows_dev, 4 * rows_dev // experts)
    slot_total = experts * capacity
    whole_experts = lax.all_gather(expert_master.astype(jnp.bfloat16), "dp", axis=2, tiled=True)
    w_up = whole_experts[0, 0]
    w_down = whole_experts[0, 1]
    dense_low = dense_master.astype(jnp.bfloat16)
    norm_low = norm_master.astype(jnp.bfloat16)
    grad_dense = jnp.zeros((4 * width, width), jnp.float32)
    grad_norm = jnp.zeros((4, width), jnp.float32)
    grad_up = jnp.zeros(w_up.shape, jnp.float32)
    grad_down = jnp.zeros(w_down.shape, jnp.float32)
    outputs_list = []
    input_list = []
    for micro in range(micro_count):
        dense_whole, norm_whole = (
            lax.all_gather(dense_low, "dp", axis=0, tiled=True),
            lax.all_gather(norm_low, "dp", axis=1, tiled=True),
        )
        norm_wide = norm_whole.astype(jnp.float32)
        block = images[micro].astype(jnp.float32).reshape(rows_dev, width)
        normed_full, normed_one, inverse_one = layer_norm(block, norm_wide[0], norm_wide[1])
        normed_one_low = normed_full.astype(jnp.bfloat16).reshape(images_here, seq, width)
        branch, kept = attention_forward(
            normed_one_low, dense_whole[: 3 * width], dense_whole[3 * width :], HEADS
        )
        residual = block + branch.reshape(rows_dev, width)
        normed_two_full, normed_two, inverse_two = layer_norm(residual, norm_wide[2], norm_wide[3])
        normed_two_low = normed_two_full.astype(jnp.bfloat16)
        index = (routes[micro] * capacity + slots[micro]).reshape(rows_dev, 2)
        gate_pair = gates[micro].reshape(rows_dev, 2)
        picks = jnp.arange(slot_total)[:, None, None] == index[None, :, :]
        dispatch = jnp.sum(picks.astype(jnp.int32), axis=2).astype(jnp.bfloat16)
        send = jnp.dot(dispatch, normed_two_low, preferred_element_type=jnp.float32).astype(
            jnp.bfloat16
        )
        received = lax.all_to_all(
            send.reshape(experts, capacity, width),
            "expert",
            split_axis=0,
            concat_axis=0,
            tiled=True,
        )
        sources, count, features = received.shape
        rows_in = received.reshape(sources * count, features)
        pre = jnp.einsum("rd,fd->rf", rows_in, w_up, preferred_element_type=jnp.float32)
        hidden = jax.nn.gelu(pre, approximate=False).astype(jnp.bfloat16)
        produced = jnp.dot(hidden, w_down, preferred_element_type=jnp.float32).astype(jnp.bfloat16)
        returned = lax.all_to_all(
            produced.reshape(sources, count, features),
            "expert",
            split_axis=0,
            concat_axis=0,
            tiled=True,
        )
        returned, received, pre = (returned, received, pre.reshape(sources, count, pre.shape[1]))
        back_flat = returned.reshape(slot_total, width)
        taken = back_flat[index].astype(jnp.float32)
        moe = gate_pair[:, 0:1] * taken[:, 0] + gate_pair[:, 1:2] * taken[:, 1]
        outputs_list.append((residual + moe).astype(jnp.bfloat16).reshape(images_here, seq, width))
        grad_output = cotangent[micro].astype(jnp.float32).reshape(rows_dev, width)
        spread = jnp.sum(jnp.where(picks, gate_pair[None, :, :], 0.0), axis=2)
        grad_send = jnp.dot(spread, grad_output, precision=HIGH).astype(jnp.bfloat16)
        grad_received = lax.all_to_all(
            grad_send.reshape(experts, capacity, width),
            "expert",
            split_axis=0,
            concat_axis=0,
            tiled=True,
        )
        grad_rows_out = grad_received.reshape(slot_total, width)
        pre_rows = pre.reshape(slot_total, pre.shape[2])
        hidden_full, gelu_pull = jax.vjp(partial(jax.nn.gelu, approximate=False), pre_rows)
        hidden = hidden_full.astype(jnp.bfloat16)
        grad_down = grad_down + jnp.einsum(
            "rf,rd->fd", hidden, grad_rows_out, preferred_element_type=jnp.float32
        )
        grad_hidden = jnp.einsum(
            "rd,fd->rf", grad_rows_out, w_down, preferred_element_type=jnp.float32
        )
        grad_pre = gelu_pull(grad_hidden)[0].astype(jnp.bfloat16)
        rows_in = received.reshape(slot_total, width)
        grad_up = grad_up + jnp.einsum(
            "rf,rd->fd", grad_pre, rows_in, preferred_element_type=jnp.float32
        )
        grad_in = jnp.dot(grad_pre, w_up, preferred_element_type=jnp.float32).astype(jnp.bfloat16)
        grad_back = lax.all_to_all(
            grad_in.reshape(experts, capacity, width),
            "expert",
            split_axis=0,
            concat_axis=0,
            tiled=True,
        )
        pair_back = grad_back.reshape(slot_total, width)[index].astype(jnp.float32)
        grad_normed_two = pair_back[:, 0] + pair_back[:, 1]
        grad_two_rows, gain_two_grad, bias_two_grad = norm_backward(
            grad_normed_two, normed_two, inverse_two, norm_wide[2]
        )
        grad_residual = grad_output + grad_two_rows
        dense_again, norm_again = (
            lax.all_gather(dense_low, "dp", axis=0, tiled=True),
            lax.all_gather(norm_low, "dp", axis=1, tiled=True),
        )
        norm_again_wide = norm_again.astype(jnp.float32)
        grad_normed_one, grad_qkv_w, grad_out_w = attention_backward(
            grad_residual.reshape(images_here, seq, width),
            normed_one_low,
            dense_again[: 3 * width],
            dense_again[3 * width :],
            kept,
            HEADS,
        )
        grad_one_rows, gain_one_grad, bias_one_grad = norm_backward(
            grad_normed_one.reshape(rows_dev, width), normed_one, inverse_one, norm_again_wide[0]
        )
        input_list.append(
            (grad_residual + grad_one_rows).astype(jnp.bfloat16).reshape(images_here, seq, width)
        )
        grad_dense = grad_dense + jnp.concatenate([grad_qkv_w, grad_out_w], axis=0)
        grad_norm = grad_norm + jnp.stack(
            [gain_one_grad, bias_one_grad, gain_two_grad, bias_two_grad]
        )
    expert_terms = jnp.stack([grad_up, grad_down])[None]
    summed_dense, summed_norm, expert_grad = (
        lax.psum_scatter(
            grad_dense.astype(jnp.bfloat16), "dp", scatter_dimension=0, tiled=True
        ).astype(jnp.float32),
        lax.psum_scatter(
            grad_norm.astype(jnp.bfloat16), "dp", scatter_dimension=1, tiled=True
        ).astype(jnp.float32),
        lax.psum_scatter(
            expert_terms.astype(jnp.bfloat16), "dp", scatter_dimension=2, tiled=True
        ).astype(jnp.float32),
    )
    dense_grad, norm_grad = (
        lax.psum(summed_dense.astype(jnp.bfloat16), "expert").astype(jnp.float32),
        lax.psum(summed_norm.astype(jnp.bfloat16), "expert").astype(jnp.float32),
    )
    return (
        jnp.stack(outputs_list),
        jnp.stack(input_list),
        dense_grad,
        norm_grad,
        expert_grad,
    )


def shards(
    images,
    cotangent,
    gates,
    routes,
    slots,
    dense_master,
    dense_momentum,
    norm_master,
    norm_momentum,
    expert_master,
    expert_momentum,
):
    micro_count, images_here, seq, width = images.shape
    experts = lax.axis_size("expert")
    dp_count = lax.axis_size("dp")
    tokens_all = micro_count * images_here * seq * dp_count * experts
    lined = dense_master.shape[0] % 128 == 0 and expert_master.shape[2] % 128 == 0
    if lined and images_here == 1 and dp_count % 2 == 0 and width == 64 * HEADS:
        out, grad, dense_grad, norm_grad, expert_grad = block(
            images, cotangent, gates, routes, dense_master, norm_master, expert_master
        )
        out, grad = out[:, None], grad[:, None]
    else:
        out, grad, dense_grad, norm_grad, expert_grad = block_plain(
            images, cotangent, gates, routes, slots, dense_master, norm_master, expert_master
        )
    norm_moment = DECAY * norm_momentum + norm_grad
    norm_new = norm_master - LR_VECTOR * tokens_all ** (-0.5) * norm_moment
    expert_moment, dense_moment, expert_new, dense_new, expert_copy, dense_copy = muon(
        expert_grad, dense_grad, expert_momentum, dense_momentum, expert_master, dense_master
    )
    return (
        out,
        grad,
        dense_grad,
        norm_grad,
        expert_grad,
        dense_moment,
        norm_moment,
        expert_moment,
        dense_new,
        norm_new,
        expert_new,
        dense_copy,
        expert_copy,
    )


def solution(mesh):
    in_specs = (
        P(None, ("dp", "expert"), None, None),
        P(None, ("dp", "expert"), None, None),
        P(None, ("dp", "expert"), None, None),
        P(None, ("dp", "expert"), None, None),
        P(None, ("dp", "expert"), None, None),
        P("dp", None),
        P("dp", None),
        P(None, "dp"),
        P(None, "dp"),
        P("expert", None, "dp", None),
        P("expert", None, "dp", None),
    )
    out_specs = (
        P(None, ("dp", "expert"), None, None),
        P(None, ("dp", "expert"), None, None),
        P("dp", None),
        P(None, "dp"),
        P("expert", None, "dp", None),
        P("dp", None),
        P(None, "dp"),
        P("expert", None, "dp", None),
        P("dp", None),
        P(None, "dp"),
        P("expert", None, "dp", None),
        P("dp", None),
        P("expert", None, "dp", None),
    )
    return jax.shard_map(shards, mesh=mesh, in_specs=in_specs, out_specs=out_specs, check_vma=False)
```

```python
from functools import partial

import jax
import jax.numpy as jnp
from jax import lax
from jax.experimental import pallas as pl
from jax.experimental.pallas import tpu as pltpu
from jax.sharding import PartitionSpec as P

MESH = pl.DeviceIdType.MESH
NT = (((1,), (1,)), ((), ()))
TN = (((0,), (0,)), ((), ()))
ERF_P = 0.3275911 * 0.5**0.5
ERF_1 = 0.254829592
ERF_2 = -0.284496736
ERF_3 = 1.421413741
ERF_4 = -1.453152027
ERF_5 = 1.061405429
ROOT_TWO_PI = 0.3989422804014327

HEADS = 8


HIGH = lax.Precision.HIGHEST
NORM_EPS = 1e-06
ORTHO_EPS = 1e-07
NS_A = 3.4445
NS_B = -4.775
NS_C = 2.0315
DECAY = 0.5
LR_QKV = 0.5
LR_OUT = 1.5
LR_EXPERT = 0.5
LR_VECTOR = 0.05


def layer_norm(rows, norm_gain, norm_bias):
    row_mean = jnp.mean(rows, axis=-1, keepdims=True)
    centred = rows - row_mean
    variance = jnp.mean(centred * centred, axis=-1, keepdims=True)
    inverse = lax.rsqrt(variance + NORM_EPS)
    normed = centred * inverse
    return (normed * norm_gain + norm_bias, normed, inverse)


def norm_backward(grad_out, normed, inverse, norm_gain):
    grad_gain = jnp.sum(grad_out * normed, axis=0)
    grad_bias = jnp.sum(grad_out, axis=0)
    scaled = grad_out * norm_gain
    grad_rows = inverse * (
        scaled
        - jnp.mean(scaled, axis=-1, keepdims=True)
        - normed * jnp.mean(scaled * normed, axis=-1, keepdims=True)
    )
    return (grad_rows, grad_gain, grad_bias)


def split_heads(projected, heads):
    images_here, seq, triple = projected.shape
    head_size = triple // (3 * heads)
    parts = projected.reshape(images_here, seq, 3, heads, head_size)
    return (parts[:, :, 0], parts[:, :, 1], parts[:, :, 2], head_size ** (-0.5))


def attention_forward(normed_low, w_qkv, w_out, heads):
    images_here, seq, width = normed_low.shape
    projected = jnp.einsum(
        "bsd,ed->bse", normed_low, w_qkv, preferred_element_type=jnp.float32
    ).astype(jnp.bfloat16)
    query_part, key_part, value_part, score_scale = split_heads(projected, heads)
    scores = (
        jnp.einsum("bqhd,bkhd->bhqk", query_part, key_part, preferred_element_type=jnp.float32)
        * score_scale
    )
    top = jnp.max(scores, axis=-1, keepdims=True)
    expo = jnp.exp(scores - top)
    total = jnp.sum(expo, axis=-1, keepdims=True)
    soft_weights = expo / total
    log_total = top + jnp.log(total)
    mixed = jnp.einsum(
        "bhqk,bkhd->bqhd",
        soft_weights.astype(jnp.bfloat16),
        value_part,
        preferred_element_type=jnp.float32,
    )
    mixed = mixed.astype(jnp.bfloat16).reshape(images_here, seq, width)
    branch = jnp.einsum("bsd,ed->bse", mixed, w_out, preferred_element_type=jnp.float32)
    return (branch, (projected, log_total, mixed))


def attention_backward(grad_branch, normed_low, w_qkv, w_out, kept, heads):
    projected, log_total, mixed = kept
    images_here, seq, width = normed_low.shape
    query_part, key_part, value_part, score_scale = split_heads(projected, heads)
    grad_low = grad_branch.astype(jnp.bfloat16)
    grad_out_w = jnp.einsum("bse,bsd->ed", grad_low, mixed, preferred_element_type=jnp.float32)
    grad_mixed = jnp.einsum(
        "bse,ed->bsd", grad_low, w_out, preferred_element_type=jnp.float32
    ).astype(jnp.bfloat16)
    grad_mixed = grad_mixed.reshape(query_part.shape)
    scores = (
        jnp.einsum("bqhd,bkhd->bhqk", query_part, key_part, preferred_element_type=jnp.float32)
        * score_scale
    )
    soft_weights = jnp.exp(scores - log_total)
    soft_low = soft_weights.astype(jnp.bfloat16)
    grad_soft = jnp.einsum(
        "bqhd,bkhd->bhqk", grad_mixed, value_part, preferred_element_type=jnp.float32
    )
    grad_scores = (
        soft_weights * (grad_soft - jnp.sum(soft_weights * grad_soft, axis=-1, keepdims=True))
    ).astype(jnp.bfloat16)
    grad_query = (
        jnp.einsum("bhqk,bkhd->bqhd", grad_scores, key_part, preferred_element_type=jnp.float32)
        * score_scale
    )
    grad_key = (
        jnp.einsum("bhqk,bqhd->bkhd", grad_scores, query_part, preferred_element_type=jnp.float32)
        * score_scale
    )
    grad_value = jnp.einsum(
        "bhqk,bqhd->bkhd", soft_low, grad_mixed, preferred_element_type=jnp.float32
    )
    grad_projected = (
        jnp.stack([grad_query, grad_key, grad_value], axis=2)
        .reshape(images_here, seq, 3 * width)
        .astype(jnp.bfloat16)
    )
    grad_qkv_w = jnp.einsum(
        "bse,bsd->ed", grad_projected, normed_low, preferred_element_type=jnp.float32
    )
    grad_normed = jnp.einsum(
        "bse,ed->bsd", grad_projected, w_qkv, preferred_element_type=jnp.float32
    )
    return (grad_normed, grad_qkv_w, grad_out_w)


def muon_kernel(
    n_dp, width, expert_grad, dense_grad, expert_momentum, dense_momentum, expert_master,
    dense_master, expert_moment, dense_moment, expert_new, dense_new, expert_copy, dense_copy,
    outgoing, held, wide, low, blend, back, send_sem, take_sem, return_sem, back_sem,
):
    me = lax.axis_index("dp")
    rows = dense_grad.shape[0]
    turned = rows % 128 == 0

    def turn_over(block):
        return block.T if turned else block

    def slot(ref, place):
        where = pl.ds(pl.multiple_of(place * rows, rows), rows)
        return ref.at[:, where] if turned else ref.at[where, :]

    query_devices = 3 * width // rows
    own_up, own_down, own_query, own_out = 0, 3 * n_dp // 4, n_dp // 4, n_dp // 2
    dense_owner = jnp.where(me < query_devices, own_query, own_out)
    dense_place = jnp.where(me < query_devices, me, me - query_devices)
    barrier = pltpu.get_barrier_semaphore()
    for step in range(1, n_dp):
        pl.semaphore_signal(
            barrier, inc=1, device_id={"dp": lax.rem(me + step, n_dp)}, device_id_type=MESH
        )
    for job in range(2):
        moment = DECAY * expert_momentum[0, job] + expert_grad[0, job]
        expert_moment[0, job] = moment
        outgoing[job] = turn_over(moment.astype(jnp.bfloat16))
    moment = DECAY * dense_momentum[...] + dense_grad[...]
    dense_moment[...] = moment
    outgoing[2] = turn_over(moment.astype(jnp.bfloat16))
    pl.semaphore_wait(barrier, n_dp - 1)

    owners = (own_up, own_down, dense_owner)
    places = (me, me, dense_place)
    for job in range(3):
        @pl.when(me != owners[job])
        def _():
            pltpu.make_async_remote_copy(
                src_ref=outgoing.at[job], dst_ref=slot(held, places[job]),
                send_sem=send_sem.at[job], recv_sem=take_sem.at[me],
                device_id={"dp": owners[job]}, device_id_type=MESH,
            ).start()

        @pl.when(me == owners[job])
        def _():
            slot(held, places[job])[...] = outgoing[job]

    def take(source):
        @pl.when(me != source)
        def _():
            pltpu.make_async_remote_copy(
                src_ref=outgoing.at[0], dst_ref=slot(held, 0),
                send_sem=send_sem.at[0], recv_sem=take_sem.at[source],
                device_id={"dp": source}, device_id_type=MESH,
            ).wait_recv()

    query_rows = 3 * width
    out_rows = n_dp * rows - query_rows
    total = n_dp * rows

    def clear(first):
        zeros = jnp.zeros((total - first, width), jnp.bfloat16)
        if turned:
            held[:, first:] = zeros.T
        else:
            held[first:, :] = zeros

    def columns(start):
        where = slice(start, start + width)
        return (held[:, where] if turned else held[where, :].T).astype(jnp.float32)

    @pl.when((me == own_up) | (me == own_down))
    def _():
        for source in range(n_dp):
            take(source)

    @pl.when(me == own_query)
    def _():
        clear(query_rows)
        for source in range(query_devices):
            take(source)

    @pl.when(me == own_out)
    def _():
        clear(out_rows)
        for source in range(query_devices, n_dp):
            take(source)

    owner = (me == own_up) | (me == own_down) | (me == own_query) | (me == own_out)

    @pl.when(owner)
    def _():
        square = jnp.zeros((1, 1), jnp.float32)
        for start in range(0, total, width):
            part = columns(start)
            square = square + jnp.sum(part * part, keepdims=True)
        scale = 1.0 / (jnp.sqrt(square) + ORTHO_EPS)
        for start in range(0, total, width):
            part = columns(start) * scale
            wide[:, start : start + width] = part
            low[:, start : start + width] = part.astype(jnp.bfloat16)

        def turn(_, carry):
            gram = lax.dot_general(low[...], low[...], NT, preferred_element_type=jnp.float32)
            gram_low = gram.astype(jnp.bfloat16)
            twice = jnp.dot(gram_low, gram_low, preferred_element_type=jnp.float32)
            blend[...] = (NS_B * gram + NS_C * twice).astype(jnp.bfloat16)

            def piece(index, inner):
                where = pl.ds(pl.multiple_of(index * width, width), width)
                part = NS_A * wide[:, where] + jnp.dot(
                    blend[...], low[:, where], preferred_element_type=jnp.float32
                )
                wide[:, where] = part
                low[:, where] = part.astype(jnp.bfloat16)
                return inner

            return lax.fori_loop(0, total // width, piece, carry)

        lax.fori_loop(0, 5, turn, 0)
        if not turned:
            for start in range(0, total, width):
                held[start : start + width, :] = low[:, start : start + width].T

    result = low if turned else held

    def give(job, target, place):
        @pl.when(me != target)
        def _():
            pltpu.make_async_remote_copy(
                src_ref=slot(result, place), dst_ref=back.at[job],
                send_sem=return_sem.at[target], recv_sem=back_sem.at[job],
                device_id={"dp": target}, device_id_type=MESH,
            ).start()

        @pl.when(me == target)
        def _():
            back[job] = slot(result, place)[...]

    def gave(target):
        @pl.when(me != target)
        def _():
            pltpu.make_async_remote_copy(
                src_ref=slot(result, 0), dst_ref=back.at[0],
                send_sem=return_sem.at[target], recv_sem=back_sem.at[0],
                device_id={"dp": target}, device_id_type=MESH,
            ).wait_send()

    jobs = (
        (own_up, 0, 0, n_dp),
        (own_down, 1, 0, n_dp),
        (own_query, 2, 0, query_devices),
        (own_out, 2, query_devices, n_dp),
    )
    for who, job, first, last in jobs:
        @pl.when(me == who)
        def _():
            for target in range(first, last):
                give(job, target, target - first)
    rates = (LR_EXPERT, LR_EXPERT, jnp.where(me < query_devices, LR_QKV, LR_OUT))
    for job in (2, 0, 1):
        @pl.when(me != owners[job])
        def _():
            pltpu.make_async_remote_copy(
                src_ref=outgoing.at[job], dst_ref=back.at[job],
                send_sem=send_sem.at[job], recv_sem=back_sem.at[job],
                device_id={"dp": owners[job]}, device_id_type=MESH,
            ).wait()

        step = rates[job] * turn_over(back[job]).astype(jnp.float32)
        if job == 2:
            new = dense_master[...] - step
            dense_new[...] = new
            dense_copy[...] = new.astype(jnp.bfloat16)
        else:
            new = expert_master[0, job] - step
            expert_new[0, job] = new
            expert_copy[0, job] = new.astype(jnp.bfloat16)
    for who, job, first, last in jobs:
        @pl.when(me == who)
        def _():
            for target in range(first, last):
                gave(target)


def muon(expert_grad, dense_grad, expert_momentum, dense_momentum, expert_master, dense_master):
    n_dp = lax.axis_size("dp")
    rows, width = dense_grad.shape
    total = n_dp * rows
    block = (width, rows) if rows % 128 == 0 else (rows, width)
    whole = (width, total) if rows % 128 == 0 else (total, width)
    full = jax.ShapeDtypeStruct(expert_grad.shape, jnp.float32)
    flat = jax.ShapeDtypeStruct(dense_grad.shape, jnp.float32)
    vmem = pl.BlockSpec(memory_space=pltpu.VMEM)
    return pl.pallas_call(
        partial(muon_kernel, n_dp, width),
        out_shape=(
            full, flat, full, flat,
            jax.ShapeDtypeStruct(expert_grad.shape, jnp.bfloat16),
            jax.ShapeDtypeStruct(dense_grad.shape, jnp.bfloat16),
        ),
        in_specs=[vmem] * 6,
        out_specs=[vmem] * 6,
        scratch_shapes=[
            pltpu.VMEM((3, *block), jnp.bfloat16),
            pltpu.VMEM(whole, jnp.bfloat16),
            pltpu.VMEM((width, total), jnp.float32),
            pltpu.VMEM((width, total), jnp.bfloat16),
            pltpu.VMEM((width, width), jnp.bfloat16),
            pltpu.VMEM((3, *block), jnp.bfloat16),
            pltpu.SemaphoreType.DMA((3,)),
            pltpu.SemaphoreType.DMA((n_dp,)),
            pltpu.SemaphoreType.DMA((n_dp,)),
            pltpu.SemaphoreType.DMA((3,)),
        ],
        compiler_params=pltpu.CompilerParams(
            collective_id=1, has_side_effects=True, vmem_limit_bytes=48 * 1024 * 1024
        ),
        name="muon",
    )(expert_grad, dense_grad, expert_momentum, dense_momentum, expert_master, dense_master)


def nn(a, b):
    return jnp.dot(a, b, preferred_element_type=jnp.float32)


def nt(a, b):
    return lax.dot_general(a, b, NT, preferred_element_type=jnp.float32)


def tn(a, b):
    return lax.dot_general(a, b, TN, preferred_element_type=jnp.float32)


def gelu_parts(pre):
    bell = jnp.exp(-0.5 * pre * pre)
    share = 1.0 / (1.0 + ERF_P * jnp.abs(pre))
    series = share * (ERF_1 + share * (ERF_2 + share * (ERF_3 + share * (ERF_4 + share * ERF_5))))
    tail = 0.5 * series * bell
    return jnp.where(pre >= 0.0, 1.0 - tail, tail), bell * ROOT_TWO_PI


def row_stats(rows):
    mean = jnp.mean(rows, axis=-1, keepdims=True)
    centred = rows - mean
    inverse = lax.rsqrt(jnp.mean(centred * centred, axis=-1, keepdims=True) + NORM_EPS)
    return centred * inverse, inverse


def rows_backward(grad_out, normed, inverse, gain):
    scaled = grad_out * gain
    return inverse * (
        scaled
        - jnp.mean(scaled, axis=-1, keepdims=True)
        - normed * jnp.mean(scaled * normed, axis=-1, keepdims=True)
    )


def block_kernel(
    cfg, images, cotangent, gates, routes, dense_master, norm_master, expert_master, dense_momentum, expert_momentum,
    activations, input_grad, dense_grad, norm_grad, expert_grad, directions,
    dense, experts, norm_slots, norms, tokens, outer_low, normed_low, projected, soft, mixed, residual,
    rows_x, rows_dy, turned_x, turned_dy, weight_slots, hidden_a, hidden_b, grad_pre_a, grad_pre_b, pre_a, pre_b, down_a, down_b,
    produced_sum, grad_in_sum, produced_out, grad_in_out, produced_mid, grad_in_mid, produced_got, grad_in_got,
    expert_sum, pair_out, pair_got, chip_got, grad_projected, grad_branch,
    dense_sum, dense_out, dense_got, dense_chip, line_out, line_got, line_all, norm_all, norm_line,
    outgoing, held, directions_got,
    dense_send, dense_take, expert_send, expert_take, norm_send, norm_take,
    dy_send, dy_take, weight_send, weight_take, x_send, x_take, g_send, g_take, gm_send, gm_take, p_send, p_take, pm_send, pm_take,
    pair_send, pair_take, chip_send, chip_take, dpair_send, dpair_take, dchip_send, dchip_take,
    line_send, line_take, lall_send, lall_take, nall_send, nall_take, nline_send, nline_take,
    row_send, row_take, return_send, return_take,
):
    n_dp, n_ex, micro_count, seq, pad, width, heads = cfg
    me, spot = lax.axis_index("dp"), lax.axis_index("expert")
    core = lax.rem(me, 2)
    partner = me + 1 - 2 * core
    chips = n_dp // 2
    chip = me // 2
    bf16 = jnp.bfloat16
    shard = expert_master.shape[2]
    dense_shard = dense_master.shape[0]
    norm_shard = norm_master.shape[1]
    near = n_ex // 2
    half_rows = near * pad
    head_size = width // heads
    score_scale = head_size ** (-0.5)

    def copy(src, dst, send, take, device):
        return pltpu.make_async_remote_copy(
            src_ref=src, dst_ref=dst, send_sem=send, recv_sem=take,
            device_id=device, device_id_type=MESH,
        )

    def over_dp(step):
        return lax.rem(me + step, n_dp)

    def over_ex(step):
        return lax.rem(spot + step, n_ex)

    def mirror(index, distance):
        other, bit = index, 1
        while bit <= distance:
            if distance // bit % 2:
                other = other + bit - 2 * bit * (index // bit % 2)
            bit *= 2
        return other

    def peer(distance):
        return mirror(spot, distance)

    def at_row(ref, index, size):
        return ref.at[pl.ds(pl.multiple_of(index * size, size), size)]

    barrier = pltpu.get_barrier_semaphore()
    for step in range(1, n_dp):
        pl.semaphore_signal(barrier, inc=1, device_id={"dp": over_dp(step)}, device_id_type=MESH)
    for step in range(1, n_ex):
        pl.semaphore_signal(barrier, inc=1, device_id={"expert": over_ex(step)}, device_id_type=MESH)

    at_row(dense, me, dense_shard)[...] = dense_master[...].astype(bf16)
    for job in range(2):
        at_row(experts.at[job], me, shard)[...] = expert_master[0, job].astype(bf16)
    norm_slots[me] = jnp.zeros(norm_slots.shape[1:], jnp.float32)
    norm_slots[me, 0:4, 0:norm_shard] = norm_master[...].astype(bf16).astype(jnp.float32)
    expert_row = lax.broadcasted_iota(jnp.int32, (weight_slots.shape[2], seq), 0)
    for micro in range(micro_count):
        weight_slots[0, micro] = jnp.zeros(weight_slots.shape[2:], jnp.float32)
        weight_slots[0, micro, :, 0:seq] = jnp.where(expert_row == routes[micro, 0:1], gates[micro, 0:1], 0.0) + jnp.where(
            expert_row == routes[micro, 1:2], gates[micro, 1:2], 0.0
        )
    tail = seq // 16 * 16
    for micro in range(micro_count):
        tokens[micro, tail:] = jnp.zeros((pad - tail, width), bf16)
        tokens[micro, 0:seq] = images[micro]
        outer_low[micro, tail:] = jnp.zeros((pad - tail, width), bf16)
        outer_low[micro, 0:seq] = cotangent[micro]
        rows_dy[micro, 0, 0:pad] = outer_low[micro]
        for side in range(2):
            rows_x[micro, side, half_rows:] = jnp.zeros((rows_x.shape[2] - half_rows, width), bf16)
            rows_dy[micro, side, half_rows:] = jnp.zeros((rows_x.shape[2] - half_rows, width), bf16)
    for buffer in (hidden_a, hidden_b, grad_pre_a, grad_pre_b):
        buffer[half_rows:] = jnp.zeros((rows_x.shape[2] - half_rows, shard), bf16)
    total_rows = held.shape[1]
    query_devices = 3 * width // dense_shard
    own_up, own_down, own_query, own_out = 0, 3 * n_dp // 4, n_dp // 4, n_dp // 2
    dense_owner = jnp.where(me < query_devices, own_query, own_out)
    dense_place = jnp.where(me < query_devices, me, me - query_devices)

    @pl.when(me == own_query)
    def _():
        held[:, 3 * width :] = jnp.zeros((width, total_rows - 3 * width), bf16)

    @pl.when(me == own_out)
    def _():
        held[:, n_dp * dense_shard - 3 * width :] = jnp.zeros((width, total_rows - n_dp * dense_shard + 3 * width), bf16)

    pl.semaphore_wait(barrier, n_dp + n_ex - 2)

    first_axis, second_axis = 1 + core, 2 - core

    def axis_chip(axis):
        return jnp.where(axis == 1, mirror(chip, 1), mirror(chip, 2))

    near_chip, next_chip, far_chip = axis_chip(first_axis), axis_chip(second_axis), mirror(chip, 3)
    sources = [2 * place + core for place in (near_chip, next_chip, far_chip)]

    def gather_start(views, send, take):
        for step, target in ((1, sources[0]), (2, sources[1]), (0, partner)):
            for k, view in enumerate(views):
                copy(view(me), view(me), send.at[k, step], take.at[k, me], {"dp": target}).start()

    def gather_got(views, send, take, source):
        for k, view in enumerate(views):
            copy(view(source), view(source), send.at[k, 0], take.at[k, source], {"dp": partner}).wait_recv()

    def gather_pass(views, send, take, which):
        source = sources[which]
        gather_got(views, send, take, source)
        for k, view in enumerate(views):
            if which == 0:
                copy(view(source), view(source), send.at[k, 3], take.at[k, source], {"dp": sources[1]}).start()
            copy(view(source), view(source), send.at[k, 4 + which], take.at[k, source], {"dp": partner}).start()

    def gather_sent(views, send, take):
        for step in range(7):
            for k, view in enumerate(views):
                copy(view(me), view(me), send.at[k, step], take.at[k, me], {"dp": partner}).wait_send()

    dense_views = [lambda i: at_row(dense, i, dense_shard)]
    expert_views = [lambda i, job=job: at_row(experts.at[job], i, shard) for job in range(2)]
    for step in range(1, n_dp):
        copy(norm_slots.at[me], norm_slots.at[me], norm_send.at[step], norm_take.at[me], {"dp": over_dp(step)}).start()
    gather_start(dense_views, dense_send, dense_take)

    def line(ref, micro, slot):
        first = slot % near * pad
        return ref.at[micro, slot // near, first : first + pad]

    def half(ref, micro, side, slot):
        return ref.at[micro, side, slot * pad : (slot + 1) * pad]

    def spread(ref, micro, send, take, slots):
        for slot in slots:
            copy(line(ref, micro, 0), line(ref, micro, slot), send.at[micro, slot], take.at[micro, slot], {"expert": peer(slot)}).start()

    def spread_got(ref, micro, send, take, slot):
        copy(line(ref, micro, 0), line(ref, micro, slot), send.at[micro, slot], take.at[micro, slot], {"expert": peer(slot)}).wait_recv()

    def spread_pass(ref, micro, send, take):
        spread_got(ref, micro, send, take, near)
        for slot in range(1, near):
            copy(line(ref, micro, near), line(ref, micro, near + slot), send.at[micro, near + slot], take.at[micro, near + slot], {"expert": peer(slot)}).start()

    def spread_sent(ref, micro, send, take, slots):
        for slot in slots:
            copy(line(ref, micro, 0), line(ref, micro, slot), send.at[micro, slot], take.at[micro, slot], {"expert": peer(1)}).wait_send()

    near_slots, far_slots = range(1, near), (near,)
    for slot in range(1, n_ex):
        copy(weight_slots.at[0], weight_slots.at[slot], weight_send.at[slot], weight_take.at[slot], {"expert": peer(slot)}).start()
    spread(rows_dy, 0, dy_send, dy_take, far_slots)
    spread(rows_dy, 0, dy_send, dy_take, near_slots)

    for step in range(1, n_dp):
        source = over_dp(step)
        copy(norm_slots.at[source], norm_slots.at[source], norm_send.at[step], norm_take.at[source], {"dp": source}).wait()
    lane = lax.broadcasted_iota(jnp.int32, (128, width), 0)
    column = lax.broadcasted_iota(jnp.int32, (128, width), 1)
    wide = jnp.zeros((8, width), jnp.float32)
    for index in range(n_dp):
        pick = ((column - norm_shard * index == lane) & (lane < norm_shard)).astype(jnp.float32).astype(bf16)
        wide = wide + nn(norm_slots[index].astype(bf16), pick)
    norms[...] = wide

    gather_pass(dense_views, dense_send, dense_take, 0)
    gather_pass(dense_views, dense_send, dense_take, 1)
    spread_pass(rows_dy, 0, dy_send, dy_take)
    spread(rows_dy, 1, dy_send, dy_take, far_slots)
    gather_pass(dense_views, dense_send, dense_take, 2)
    gather_start(expert_views, expert_send, expert_take)
    for place in (chip, mirror(chip, 1), mirror(chip, 2), far_chip):
        gather_got(dense_views, dense_send, dense_take, 2 * place + 1 - core)

    left = lax.broadcasted_iota(jnp.int32, (pad, 128), 1) < head_size
    low_masks = [left.astype(jnp.float32).astype(bf16), (1.0 - left.astype(jnp.float32)).astype(bf16)]
    real_key = lax.broadcasted_iota(jnp.int32, (pad, pad), 1) < seq

    def pair_of(micro, part, index):
        first = part * width + index * 128
        return projected[micro, :, first : first + 128]

    def attend(micro, carry):
        normed, _ = row_stats(tokens[micro].astype(jnp.float32))
        low = (normed * norms[0:1] + norms[1:2]).astype(bf16)
        normed_low[micro] = low
        projected[micro] = nt(low, dense[0 : 3 * width]).astype(bf16)
        for index in range(heads // 2):
            query, key, value = (pair_of(micro, part, index) for part in range(3))
            parts = []
            for side in range(2):
                scores = nt(query * low_masks[side], key) * score_scale
                scores = jnp.where(real_key, scores, -1e30)
                top = jnp.max(scores, axis=-1, keepdims=True)
                expo = jnp.exp(scores - top)
                weight = expo / jnp.sum(expo, axis=-1, keepdims=True)
                soft[micro, 2 * index + side] = weight
                parts.append(nn(weight.astype(bf16), value))
            mixed[micro, :, index * 128 : (index + 1) * 128] = jnp.where(left, parts[0], parts[1]).astype(bf16)
        total = tokens[micro].astype(jnp.float32) + nt(mixed[micro], dense[3 * width :])
        residual[micro] = total
        normed, _ = row_stats(total)
        rows_x[micro, 0, 0:pad] = (normed * norms[2:3] + norms[3:4]).astype(bf16)

        @pl.when(micro == 0)
        def _():
            spread(rows_x, 0, x_send, x_take, near_slots)

        return carry

    lax.fori_loop(0, micro_count, attend, 0)
    spread(rows_x, 0, x_send, x_take, far_slots)
    spread_pass(rows_dy, 1, dy_send, dy_take)
    for slot in range(1, n_ex):
        copy(weight_slots.at[0], weight_slots.at[slot], weight_send.at[slot], weight_take.at[slot], {"expert": peer(slot)}).wait()

    def column_of(slot, micro, row):
        picked = jnp.broadcast_to(weight_slots[slot, micro, pl.ds(row, 1)], (8, weight_slots.shape[3]))
        return picked.T[0:pad, 0:1]

    def back_near(out, got, micro, send, take):
        for slot in range(1, near):
            copy(line(out, micro, slot), got.at[micro, slot - 1], send.at[micro, slot], take.at[micro, slot], {"expert": peer(slot)}).start()

    def back_far(out, mid, micro, send, take):
        for slot in range(1, near):
            copy(line(out, micro, near + slot), mid.at[micro, slot - 1], send.at[micro, slot], take.at[micro, slot], {"expert": peer(slot)}).start()

    def back_join(out, mid, got, micro, mid_send, mid_take, send, take):
        total = line(out, micro, near)[...].astype(jnp.float32)
        for slot in range(1, near):
            copy(line(out, micro, near + slot), mid.at[micro, slot - 1], mid_send.at[micro, slot], mid_take.at[micro, slot], {"expert": peer(slot)}).wait()
            total = total + mid[micro, slot - 1].astype(jnp.float32)
        line(out, micro, near)[...] = total.astype(bf16)
        copy(line(out, micro, near), got.at[micro, near - 1], send.at[micro, near], take.at[micro, near], {"expert": peer(near)}).start()

    def back_got(out, got, micro, send, take):
        total = out[micro, 0, 0:pad].astype(jnp.float32)
        for slot in range(1, near + 1):
            where = out.at[micro, 0, 0:pad]
            copy(where, got.at[micro, slot - 1], send.at[micro, slot], take.at[micro, slot], {"expert": peer(slot)}).wait()
            total = total + got[micro, slot - 1].astype(jnp.float32)
        return total

    step_count = 2 * micro_count
    join_g = lambda micro: back_join(grad_in_out, grad_in_mid, grad_in_got, micro, gm_send, gm_take, g_send, g_take)
    join_p = lambda micro: back_join(produced_out, produced_mid, produced_got, micro, pm_send, pm_take, p_send, p_take)

    def pair_copy(turn, place):
        return copy(pair_out.at[lax.rem(turn, 2)], pair_got.at[place], pair_send.at[place], pair_take.at[place], {"dp": partner})

    def chip_step(turn, place):
        index = 2 * place + core
        pair_copy(turn, place).wait()
        for job in range(2):
            pair_got[place, job] = (expert_sum[index, job] + pair_got[place, job].astype(jnp.float32)).astype(bf16)
        copy(pair_got.at[place], chip_got.at[chip], chip_send.at[place], chip_take.at[chip], {"dp": index}).start()

    def send_pair(turn, place):
        pair_out[lax.rem(turn, 2)] = expert_sum[2 * place + 1 - core].astype(bf16)
        pair_copy(turn, place).start()

    expert_sum[...] = jnp.zeros(expert_sum.shape, jnp.float32)

    def run_step(number, nothing):
        micro = number // 2
        side = lax.rem(micro + number, 2)
        first, last = number == 0, number == step_count - 1
        for slot in range(1, near):
            for ref, send, take in ((rows_dy, dy_send, dy_take), (rows_x, x_send, x_take)):
                copy(half(ref, micro, side, 0), half(ref, micro, side, slot), send.at[micro, slot], take.at[micro, side * near + slot], {"expert": peer(slot)}).wait_recv()

        @pl.when(side == 0)
        def _():
            spread_sent(rows_dy, micro, dy_send, dy_take, range(1, near + 1))

        @pl.when(side == 1)
        def _():
            spread_sent(rows_dy, micro, dy_send, dy_take, range(near + 1, n_ex))

        @pl.when(first)
        def _():
            gather_pass(expert_views, expert_send, expert_take, 0)
            gather_got(expert_views, expert_send, expert_take, partner)

        gates = [column_of(side * near + slot, micro, spot) for slot in range(near)]
        for slot in range(near):
            where = half(rows_dy, micro, side, slot)
            where[...] = (gates[slot] * where[...].astype(jnp.float32)).astype(bf16)
        turned_x[...] = rows_x[micro, side].T
        turned_dy[...] = rows_dy[micro, side].T
        produced_sum[...] = jnp.zeros(produced_sum.shape, jnp.float32)
        grad_in_sum[...] = jnp.zeros(grad_in_sum.shape, jnp.float32)

        def place_of(turn):
            turn = jnp.where(last, lax.rem(turn + 1, chips), turn)
            along = jnp.where(
                turn == 1, jnp.where(last, mirror(chip, 1), near_chip), jnp.where(last, mirror(chip, 2), next_chip)
            )
            return jnp.where(turn == 0, chip, jnp.where(turn == 3, far_chip, along))

        def index_of(turn, second):
            return 2 * place_of(turn) + jnp.where(last, second, lax.rem(core + second, 2))

        def enter(index, pre, down):
            pre[...] = nt(rows_x[micro, side, 0:half_rows], at_row(experts.at[0], index, shard)[...])
            down[...] = nt(rows_dy[micro, side, 0:half_rows], at_row(experts.at[1], index, shard)[...])

        def bend(pre, down, hidden, grad_pre):
            value = pre[...]
            below, density = gelu_parts(value)
            hidden[0:half_rows] = (value * below).astype(bf16)
            grad_pre[0:half_rows] = (down[...] * (below + value * density)).astype(bf16)

        def leave(index, hidden, grad_pre):
            produced_sum[...] += nn(hidden[0:half_rows], at_row(experts.at[1], index, shard)[...])
            grad_in_sum[...] += nn(grad_pre[0:half_rows], at_row(experts.at[0], index, shard)[...])
            expert_sum[index, 0] += nn(turned_x[...], grad_pre[...])
            expert_sum[index, 1] += nn(turned_dy[...], hidden[...])

        def two_chunks(turn, carry):
            @pl.when(first & (turn < chips - 2))
            def _():
                gather_got(expert_views, expert_send, expert_take, 2 * jnp.where(turn == 0, next_chip, far_chip) + core)

            for step, when, event in events:
                pl.when((number == step) & (turn == when))(event)

            @pl.when(first)
            def _():
                gather_got(expert_views, expert_send, expert_take, 2 * place_of(turn + 1) + 1 - core)

            bend(pre_b, down_b, hidden_b, grad_pre_b)
            enter(index_of(turn + 1, 0), pre_a, down_a)
            leave(index_of(turn, 0), hidden_a, grad_pre_a)
            bend(pre_a, down_a, hidden_a, grad_pre_a)
            enter(index_of(turn + 1, 1), pre_b, down_b)
            leave(index_of(turn, 1), hidden_b, grad_pre_b)

            @pl.when(last)
            def _():
                send_pair(turn, place_of(turn))

            @pl.when(last & (turn > 0))
            def _():
                chip_step(turn - 1, place_of(turn - 1))
            return carry

        def pass_expert(which):
            source = sources[which]
            for k, view in enumerate(expert_views):
                copy(view(source), view(source), expert_send.at[k, 4 + which], expert_take.at[k, source], {"dp": partner}).start()

        events = [
            (0, 0, partial(pass_expert, 1)),
            (0, 1, partial(pass_expert, 2)),
            (0, 1, partial(spread_pass, rows_x, 0, x_send, x_take)),
            (0, 1, partial(spread, rows_x, 1, x_send, x_take, far_slots)),
            (1, 0, partial(spread_pass, rows_x, 1, x_send, x_take)),
            (1, 1, partial(spread, rows_dy, 1, dy_send, dy_take, near_slots)),
            (1, 1, partial(spread, rows_x, 1, x_send, x_take, near_slots)),
            (2, 2, partial(join_g, 0)),
            (3, 1, partial(join_g, 1)),
        ]
        enter(index_of(0, 0), pre_a, down_a)
        bend(pre_a, down_a, hidden_a, grad_pre_a)
        enter(index_of(0, 1), pre_b, down_b)
        lax.fori_loop(0, chips - 1, two_chunks, 0)
        bend(pre_b, down_b, hidden_b, grad_pre_b)
        leave(index_of(chips - 1, 0), hidden_a, grad_pre_a)
        leave(index_of(chips - 1, 1), hidden_b, grad_pre_b)

        grad_in_out[micro, side] = grad_in_sum[...].astype(bf16)
        for slot in range(near):
            half(produced_out, micro, side, slot)[...] = (gates[slot] * produced_sum[slot * pad : (slot + 1) * pad]).astype(bf16)

        @pl.when(last)
        def _():
            send_pair(chips - 1, chip)
            chip_step(chips - 2, place_of(chips - 2))

        @pl.when(side == 1)
        def _():
            back_far(grad_in_out, grad_in_mid, micro, gm_send, gm_take)

        @pl.when(lax.rem(number, 2) == 1)
        def _():
            back_near(grad_in_out, grad_in_got, micro, g_send, g_take)
        return nothing

    lax.fori_loop(0, step_count, run_step, 0)

    def attend_back(micro, carry):
        incoming = back_got(grad_in_out, grad_in_got, micro, g_send, g_take)

        @pl.when(micro == micro_count - 1)
        def _():
            for index in range(micro_count):
                back_far(produced_out, produced_mid, index, pm_send, pm_take)
                back_near(produced_out, produced_got, index, p_send, p_take)

        normed, inverse = row_stats(residual[micro])
        gain_two = jnp.sum(incoming * normed, axis=0, keepdims=True)
        bias_two = jnp.sum(incoming, axis=0, keepdims=True)
        total = outer_low[micro].astype(jnp.float32) + rows_backward(incoming, normed, inverse, norms[2:3])
        branch_low = total.astype(bf16)
        grad_branch[pl.ds(pl.multiple_of(micro * pad, 16), pad)] = branch_low
        grad_mixed = nn(branch_low, dense[3 * width :]).astype(bf16)
        for index in range(heads // 2):
            query, key, value = (pair_of(micro, part, index) for part in range(3))
            grad_pair = grad_mixed[:, index * 128 : (index + 1) * 128]
            parts = []
            for side in range(2):
                weight = soft[micro, 2 * index + side]
                grad_soft = nt(grad_pair * low_masks[side], value)
                grad_scores = (
                    weight * (grad_soft - jnp.sum(weight * grad_soft, axis=-1, keepdims=True))
                ).astype(bf16)
                parts.append((
                    nn(grad_scores, key) * score_scale,
                    tn(grad_scores, query) * score_scale,
                    tn(weight.astype(bf16), grad_pair),
                ))
            for part in range(3):
                first = part * width + index * 128
                grad_projected[pl.ds(pl.multiple_of(micro * pad, 16), pad), first : first + 128] = jnp.where(
                    left, parts[0][part], parts[1][part]
                ).astype(bf16)
        back = nn(grad_projected[pl.ds(pl.multiple_of(micro * pad, 16), pad)], dense[0 : 3 * width])
        normed, inverse = row_stats(tokens[micro].astype(jnp.float32))
        gain_one = jnp.sum(back * normed, axis=0, keepdims=True)
        bias_one = jnp.sum(back, axis=0, keepdims=True)
        total = total + rows_backward(back, normed, inverse, norms[0:1])
        input_grad[micro] = total[0:seq].astype(bf16)
        for row, part in enumerate((gain_one, bias_one, gain_two, bias_two)):
            norm_all[me, row : row + 1] += part
        return carry

    norm_all[me] = jnp.zeros((8, width), jnp.float32)
    depth = grad_branch.shape[0]
    if depth > micro_count * pad:
        grad_projected[micro_count * pad :] = jnp.zeros((depth - micro_count * pad, 3 * width), bf16)
        grad_branch[micro_count * pad :] = jnp.zeros((depth - micro_count * pad, width), bf16)
    lax.fori_loop(0, micro_count, attend_back, 0)

    for step in range(1, n_dp):
        copy(norm_all.at[me], norm_all.at[me], nall_send.at[step], nall_take.at[me], {"dp": over_dp(step)}).start()

    depth = grad_branch.shape[0]
    spare = [jnp.zeros((depth - micro_count * pad, width), bf16)] if depth > micro_count * pad else []
    turned_x[:, 0:depth] = jnp.concatenate([normed_low[micro] for micro in range(micro_count)] + spare, axis=0).T
    turned_dy[:, 0:depth] = jnp.concatenate([mixed[micro] for micro in range(micro_count)] + spare, axis=0).T

    def dense_chunk(count, carry):
        place = lax.rem(chip + 1 + count // 2, chips)
        index = 2 * place + lax.rem(count, 2)
        in_query = index * dense_shard < 3 * width

        @pl.when(in_query)
        def _():
            dense_sum[chips] = nn(turned_x[:, 0:depth], grad_projected[:, pl.ds(pl.multiple_of(jnp.where(in_query, index, 0) * dense_shard, 128), dense_shard)])

        @pl.when(jnp.logical_not(in_query))
        def _():
            first = jnp.where(in_query, 0, index * dense_shard - 3 * width)
            dense_sum[chips] = nn(turned_dy[:, 0:depth], grad_branch[:, pl.ds(pl.multiple_of(first, 128), dense_shard)])

        @pl.when(lax.rem(count, 2) == core)
        def _():
            dense_sum[place] = dense_sum[chips]

        @pl.when(lax.rem(count, 2) != core)
        def _():
            dense_out[place] = dense_sum[chips].astype(bf16)
            copy(dense_out.at[place], dense_got.at[place], dpair_send.at[place], dpair_take.at[place], {"dp": partner}).start()

        @pl.when((lax.rem(count, 2) == 1) & (count >= 3))
        def _():
            before = lax.rem(chip + count // 2, chips)
            copy(dense_out.at[before], dense_got.at[before], dpair_send.at[before], dpair_take.at[before], {"dp": partner}).wait()
            dense_got[before] = (dense_sum[before] + dense_got[before].astype(jnp.float32)).astype(bf16)
            copy(dense_got.at[before], dense_chip.at[chip], dchip_send.at[before], dchip_take.at[chip], {"dp": 2 * before + core}).start()
        return carry

    lax.fori_loop(0, n_dp, dense_chunk, 0)

    copy(dense_out.at[chip], dense_got.at[chip], dpair_send.at[chip], dpair_take.at[chip], {"dp": partner}).wait()
    plane = dense_sum[chip] + dense_got[chip].astype(jnp.float32)
    for step in range(1, chips):
        place = lax.rem(chip + step, chips)
        copy(dense_got.at[place], dense_chip.at[place], dchip_send.at[place], dchip_take.at[place], {"dp": 2 * place + core}).wait()
        plane = plane + dense_chip[place].astype(jnp.float32)
    quarter = width // n_ex
    for index in range(n_ex):
        line_out[index] = plane[index * quarter : (index + 1) * quarter].astype(bf16)
    for step in range(1, n_ex):
        target = over_ex(step)
        copy(line_out.at[target], line_got.at[spot], line_send.at[step], line_take.at[spot], {"expert": target}).start()
    for step in range(1, n_dp):
        source = over_dp(step)
        copy(norm_all.at[source], norm_all.at[source], nall_send.at[step], nall_take.at[source], {"dp": source}).wait()
    norm_total = norm_all[0]
    for index in range(1, n_dp):
        norm_total = norm_total + norm_all[index]
    norm_line[spot] = norm_total
    for step in range(1, n_ex):
        copy(norm_line.at[spot], norm_line.at[spot], nline_send.at[step], nline_take.at[spot], {"expert": over_ex(step)}).start()
    pair_copy(chips - 1, chip).wait()
    for job in range(2):
        expert_sum[me, job] = expert_sum[me, job] + pair_got[chip, job].astype(jnp.float32)
    for step in range(1, chips):
        place = lax.rem(chip + step, chips)
        copy(pair_got.at[place], chip_got.at[place], chip_send.at[place], chip_take.at[place], {"dp": 2 * place + core}).wait()
        for job in range(2):
            expert_sum[me, job] = expert_sum[me, job] + chip_got[place, job].astype(jnp.float32)
    def slot_of(ref, place, size):
        return ref.at[:, pl.ds(pl.multiple_of(place * size, size), size)]

    def row_copy(job, owner, place, size):
        return copy(outgoing.at[job], slot_of(held, place, size), row_send.at[job], row_take.at[me], {"dp": owner})

    def send_rows(job, owner, place, size):
        @pl.when(me != owner)
        def _():
            row_copy(job, owner, place, size).start()

        @pl.when(me == owner)
        def _():
            slot_of(held, place, size)[...] = outgoing[job]

    for job, owner in enumerate((own_up, own_down)):
        outgoing[job] = (DECAY * expert_momentum[0, job].T + expert_sum[me, job]).astype(bf16)
        send_rows(job, owner, me, shard)
        expert_grad[0, job] = expert_sum[me, job].T
    dense_sum[chips] = DECAY * dense_momentum[...].T

    summed = line_out[spot].astype(jnp.float32)
    for step in range(1, n_ex):
        source = over_ex(step)
        copy(line_out.at[source], line_got.at[source], line_send.at[step], line_take.at[source], {"expert": source}).wait()
        summed = summed + line_got[source].astype(jnp.float32)
    line_all[spot] = summed.astype(bf16)
    for step in range(1, n_ex):
        copy(line_all.at[spot], line_all.at[spot], lall_send.at[step], lall_take.at[spot], {"expert": over_ex(step)}).start()

    for step in range(1, n_ex):
        source = over_ex(step)
        copy(line_all.at[source], line_all.at[source], lall_send.at[step], lall_take.at[source], {"expert": source}).wait()
    for index in range(n_ex):
        where = slice(index * quarter, (index + 1) * quarter)
        outgoing[2, where] = (dense_sum[chips, where] + line_all[index].astype(jnp.float32)).astype(bf16)
    send_rows(2, dense_owner, dense_place, dense_shard)
    for micro in range(micro_count):
        join_p(micro)

    gather_sent(dense_views, dense_send, dense_take)
    gather_sent(expert_views, expert_send, expert_take)
    for micro in range(micro_count):
        spread_sent(rows_x, micro, x_send, x_take, range(1, n_ex))

    is_up, is_down, is_query, is_out = me == own_up, me == own_down, me == own_query, me == own_out
    source_first = jnp.where(is_out, query_devices, 0)
    source_count = jnp.where(is_query, query_devices, jnp.where(is_out, n_dp - query_devices, n_dp))
    job_here = jnp.where(is_up, 0, jnp.where(is_down, 1, 2))
    pieces = total_rows // width
    halves = width // shard

    def low(piece):
        return rows_x.at[piece // 2, piece % 2]

    def low_shard(place):
        first = place % halves * shard
        return low(place // halves).at[:, first : first + shard]

    blend = turned_x

    def wide(piece, part):
        return expert_sum.at[piece * halves + part, 0]

    def give(place):
        target = source_first + place

        @pl.when((place < source_count) & (me != target))
        def _():
            copy(low_shard(place), directions_got.at[job_here], return_send.at[place], return_take.at[job_here], {"dp": target}).start()

        @pl.when((place < source_count) & (me == target))
        def _():
            directions_got[job_here] = low_shard(place)[...]

    def blend_of(gram):
        gram_low = gram.astype(bf16)
        blend[...] = (NS_B * gram + NS_C * nn(gram_low, gram_low)).astype(bf16)

    @pl.when(is_up | is_down | is_query | is_out)
    def _():
        for source in range(n_dp):
            @pl.when((me != source) & (source >= source_first) & (source < source_first + source_count))
            def _():
                copy(outgoing.at[0], held.at[:, 0:shard], row_send.at[0], row_take.at[source], {"dp": source}).wait_recv()

        gram = nt(held[...], held[...])
        same = lax.broadcasted_iota(jnp.int32, (width, width), 0) == lax.broadcasted_iota(jnp.int32, (width, width), 1)
        trace = jnp.sum(jnp.sum(jnp.where(same, gram, 0.0), axis=0, keepdims=True), axis=1, keepdims=True)
        scale = 1.0 / (jnp.sqrt(trace) + ORTHO_EPS)
        blend_of(gram * (scale * scale))
        for piece in range(pieces):
            where = slice(piece * width, (piece + 1) * width)
            part = scale * (NS_A * held[:, where].astype(jnp.float32) + nn(blend[...], held[:, where]))
            low(piece)[...] = part.astype(bf16)
            for index in range(halves):
                wide(piece, index)[...] = part[:, index * shard : (index + 1) * shard]

        def turn(_, carry):
            every = jnp.concatenate([low(piece)[...] for piece in range(pieces)], axis=1)
            blend_of(nt(every, every))
            for piece in range(pieces):
                part = nn(blend[...], low(piece)[...])
                for index in range(halves):
                    fresh = NS_A * wide(piece, index)[...] + part[:, index * shard : (index + 1) * shard]
                    wide(piece, index)[...] = fresh
                    low_shard(piece * halves + index)[...] = fresh.astype(bf16)
            return carry

        lax.fori_loop(0, 4, turn, 0)
        for place in range(n_dp):
            give(place)

    for micro in range(micro_count):
        total = residual[micro] + back_got(produced_out, produced_got, micro, p_send, p_take)
        activations[micro] = total[0:seq].astype(bf16)
    for step in range(1, n_ex):
        source = over_ex(step)
        copy(norm_line.at[source], norm_line.at[source], nline_send.at[step], nline_take.at[source], {"expert": source}).wait()
    norm_total = norm_line[0]
    for index in range(1, n_ex):
        norm_total = norm_total + norm_line[index]
    for index in range(n_dp):
        @pl.when(me == index)
        def _():
            norm_grad[...] = norm_total[0:4, index * norm_shard : (index + 1) * norm_shard]
    for index in range(n_ex):
        dense_grad[:, index * quarter : (index + 1) * quarter] = line_all[index].astype(jnp.float32).T
    owners = (own_up, own_down, dense_owner)
    for job, owner in enumerate(owners):
        @pl.when(me != owner)
        def _():
            row_copy(job, owner, 0, shard).wait_send()
            copy(outgoing.at[job], directions_got.at[job], row_send.at[job], return_take.at[job], {"dp": owner}).wait_recv()

    directions[...] = directions_got[...]

    @pl.when(is_up | is_down | is_query | is_out)
    def _():
        for place in range(n_dp):
            @pl.when((place < source_count) & (me != source_first + place))
            def _():
                copy(low_shard(place), directions_got.at[0], return_send.at[place], return_take.at[0], {"dp": source_first + place}).wait_send()


def finish_kernel(
    query_devices, rate, out, grad, dense_grad, norm_grad, expert_grad, directions,
    dense_momentum, norm_momentum, expert_momentum, dense_master, norm_master, expert_master,
    out_o, grad_o, dense_grad_o, norm_grad_o, expert_grad_o, dense_moment, norm_moment, expert_moment,
    dense_new, norm_new, expert_new, dense_copy, expert_copy,
):
    for source, target in ((out, out_o), (grad, grad_o), (dense_grad, dense_grad_o), (norm_grad, norm_grad_o), (expert_grad, expert_grad_o)):
        target[...] = source[...]
    dense_moment[...] = DECAY * dense_momentum[...] + dense_grad[...]
    expert_moment[...] = DECAY * expert_momentum[...] + expert_grad[...]
    moment = DECAY * norm_momentum[...] + norm_grad[...]
    norm_moment[...] = moment
    norm_new[...] = norm_master[...] - rate * moment
    for job in range(2):
        new = expert_master[0, job] - LR_EXPERT * directions[job].astype(jnp.float32).T
        expert_new[0, job] = new
        expert_copy[0, job] = new.astype(jnp.bfloat16)
    dense_rate = jnp.where(lax.axis_index("dp") < query_devices, LR_QKV, LR_OUT)
    new = dense_master[...] - dense_rate * directions[2].astype(jnp.float32).T
    dense_new[...] = new
    dense_copy[...] = new.astype(jnp.bfloat16)


def finish(query_devices, rate, *arrays):
    out, grad, dense_grad, norm_grad, expert_grad = arrays[:5]
    f32, bf16 = jnp.float32, jnp.bfloat16
    shapes = [(out.shape, bf16), (grad.shape, bf16)]
    trio = [dense_grad.shape, norm_grad.shape, expert_grad.shape]
    shapes += [(shape, f32) for shape in trio] * 3
    shapes += [(trio[0], bf16), (trio[2], bf16)]
    vmem = pl.BlockSpec(memory_space=pltpu.VMEM)
    return pl.pallas_call(
        partial(finish_kernel, query_devices, rate),
        out_shape=tuple(jax.ShapeDtypeStruct(*shape) for shape in shapes),
        in_specs=[vmem] * len(arrays),
        out_specs=[vmem] * len(shapes),
        compiler_params=pltpu.CompilerParams(vmem_limit_bytes=67043328),
        name="finish",
    )(*arrays)


def block(images, cotangent, gates, routes, dense_master, norm_master, expert_master, dense_momentum, expert_momentum):
    micro_count, _, seq, width = images.shape
    n_dp, n_ex = lax.axis_size("dp"), lax.axis_size("expert")
    pad = -(-seq // 16) * 16
    lanes = -(-seq // 128) * 128
    shard, dense_shard, norm_shard = expert_master.shape[2], dense_master.shape[0], norm_master.shape[1]
    chips = n_dp // 2
    near = n_ex // 2
    half_rows = near * pad
    half_pad = -(-half_rows // 128) * 128
    slots = -(-n_ex // 8) * 8
    depth = -(-micro_count * pad // 128) * 128
    vmem = pl.BlockSpec(memory_space=pltpu.VMEM)
    bf16, f32 = jnp.bfloat16, jnp.float32
    dma = pltpu.SemaphoreType.DMA
    tokens = (micro_count, pad, width)
    scratch = [
        pltpu.VMEM((n_dp * dense_shard, width), bf16),
        pltpu.VMEM((2, n_dp * shard, width), bf16),
        pltpu.VMEM((n_dp, 8, 128), f32),
        pltpu.VMEM((8, width), f32),
        pltpu.VMEM(tokens, bf16),
        pltpu.VMEM(tokens, bf16),
        pltpu.VMEM(tokens, bf16),
        pltpu.VMEM((micro_count, pad, 3 * width), bf16),
        pltpu.VMEM((micro_count, HEADS, pad, pad), f32),
        pltpu.VMEM(tokens, bf16),
        pltpu.VMEM(tokens, f32),
        pltpu.VMEM((micro_count, 2, half_pad, width), bf16),
        pltpu.VMEM((micro_count, 2, half_pad, width), bf16),
        pltpu.VMEM((width, half_pad), bf16),
        pltpu.VMEM((width, half_pad), bf16),
        pltpu.VMEM((n_ex, micro_count, slots, lanes), f32),
        *[pltpu.VMEM((half_pad, shard), bf16)] * 4,
        *[pltpu.VMEM((half_rows, shard), f32)] * 4,
        pltpu.VMEM((half_rows, width), f32),
        pltpu.VMEM((half_rows, width), f32),
        pltpu.VMEM((micro_count, 2, half_rows, width), bf16),
        pltpu.VMEM((micro_count, 2, half_rows, width), bf16),
        pltpu.VMEM((micro_count, near - 1, pad, width), bf16),
        pltpu.VMEM((micro_count, near - 1, pad, width), bf16),
        pltpu.VMEM((micro_count, near, pad, width), bf16),
        pltpu.VMEM((micro_count, near, pad, width), bf16),
        pltpu.VMEM((n_dp, 2, width, shard), f32),
        pltpu.VMEM((2, 2, width, shard), bf16),
        pltpu.VMEM((chips, 2, width, shard), bf16),
        pltpu.VMEM((chips, 2, width, shard), bf16),
        pltpu.VMEM((depth, 3 * width), bf16),
        pltpu.VMEM((depth, width), bf16),
        pltpu.VMEM((chips + 1, width, dense_shard), f32),
        pltpu.VMEM((chips, width, dense_shard), bf16),
        pltpu.VMEM((chips, width, dense_shard), bf16),
        pltpu.VMEM((chips, width, dense_shard), bf16),
        pltpu.VMEM((n_ex, width // n_ex, dense_shard), bf16),
        pltpu.VMEM((n_ex, width // n_ex, dense_shard), bf16),
        pltpu.VMEM((n_ex, width // n_ex, dense_shard), bf16),
        pltpu.VMEM((n_dp, 8, width), f32),
        pltpu.VMEM((n_ex, 8, width), f32),
        pltpu.VMEM((3, width, shard), bf16),
        pltpu.VMEM((width, n_dp * shard), bf16),
        pltpu.VMEM((3, width, shard), bf16),
    ]
    sems = [(1, n_dp), (1, n_dp), (2, n_dp), (2, n_dp), (n_dp,), (n_dp,)]
    sems += [(micro_count, n_ex)] * 2 + [(n_ex,)] * 2 + [(micro_count, n_ex)] * 10
    sems += [(chips,)] * 8 + [(n_ex,)] * 4 + [(n_dp,)] * 2 + [(n_ex,)] * 2
    sems += [(3,), (n_dp,), (n_dp,), (3,)]
    cfg = (n_dp, n_ex, micro_count, seq, pad, width, HEADS)
    return pl.pallas_call(
        partial(block_kernel, cfg),
        out_shape=(
            jax.ShapeDtypeStruct((micro_count, seq, width), bf16),
            jax.ShapeDtypeStruct((micro_count, seq, width), bf16),
            jax.ShapeDtypeStruct(dense_master.shape, f32),
            jax.ShapeDtypeStruct(norm_master.shape, f32),
            jax.ShapeDtypeStruct(expert_master.shape, f32),
            jax.ShapeDtypeStruct((3, width, shard), bf16),
        ),
        in_specs=[vmem] * 9,
        out_specs=[vmem] * 6,
        scratch_shapes=scratch + [dma(shape) for shape in sems],
        compiler_params=pltpu.CompilerParams(
            collective_id=2, has_side_effects=True, vmem_limit_bytes=67043328
        ),
        name="block",
    )(
        images[:, 0], cotangent[:, 0], gates[:, 0].transpose(0, 2, 1), routes[:, 0].transpose(0, 2, 1),
        dense_master, norm_master, expert_master, dense_momentum, expert_momentum,
    )


def block_plain(images, cotangent, gates, routes, slots, dense_master, norm_master, expert_master):
    micro_count, images_here, seq, width = images.shape
    experts = lax.axis_size("expert")
    dp_count = lax.axis_size("dp")
    rows_dev = images_here * seq
    capacity = min(rows_dev, 4 * rows_dev // experts)
    slot_total = experts * capacity
    whole_experts = lax.all_gather(expert_master.astype(jnp.bfloat16), "dp", axis=2, tiled=True)
    w_up = whole_experts[0, 0]
    w_down = whole_experts[0, 1]
    dense_low = dense_master.astype(jnp.bfloat16)
    norm_low = norm_master.astype(jnp.bfloat16)
    grad_dense = jnp.zeros((4 * width, width), jnp.float32)
    grad_norm = jnp.zeros((4, width), jnp.float32)
    grad_up = jnp.zeros(w_up.shape, jnp.float32)
    grad_down = jnp.zeros(w_down.shape, jnp.float32)
    outputs_list = []
    input_list = []
    for micro in range(micro_count):
        dense_whole, norm_whole = (
            lax.all_gather(dense_low, "dp", axis=0, tiled=True),
            lax.all_gather(norm_low, "dp", axis=1, tiled=True),
        )
        norm_wide = norm_whole.astype(jnp.float32)
        block = images[micro].astype(jnp.float32).reshape(rows_dev, width)
        normed_full, normed_one, inverse_one = layer_norm(block, norm_wide[0], norm_wide[1])
        normed_one_low = normed_full.astype(jnp.bfloat16).reshape(images_here, seq, width)
        branch, kept = attention_forward(
            normed_one_low, dense_whole[: 3 * width], dense_whole[3 * width :], HEADS
        )
        residual = block + branch.reshape(rows_dev, width)
        normed_two_full, normed_two, inverse_two = layer_norm(residual, norm_wide[2], norm_wide[3])
        normed_two_low = normed_two_full.astype(jnp.bfloat16)
        index = (routes[micro] * capacity + slots[micro]).reshape(rows_dev, 2)
        gate_pair = gates[micro].reshape(rows_dev, 2)
        picks = jnp.arange(slot_total)[:, None, None] == index[None, :, :]
        dispatch = jnp.sum(picks.astype(jnp.int32), axis=2).astype(jnp.bfloat16)
        send = jnp.dot(dispatch, normed_two_low, preferred_element_type=jnp.float32).astype(
            jnp.bfloat16
        )
        received = lax.all_to_all(
            send.reshape(experts, capacity, width),
            "expert",
            split_axis=0,
            concat_axis=0,
            tiled=True,
        )
        sources, count, features = received.shape
        rows_in = received.reshape(sources * count, features)
        pre = jnp.einsum("rd,fd->rf", rows_in, w_up, preferred_element_type=jnp.float32)
        hidden = jax.nn.gelu(pre, approximate=False).astype(jnp.bfloat16)
        produced = jnp.dot(hidden, w_down, preferred_element_type=jnp.float32).astype(jnp.bfloat16)
        returned = lax.all_to_all(
            produced.reshape(sources, count, features),
            "expert",
            split_axis=0,
            concat_axis=0,
            tiled=True,
        )
        returned, received, pre = (returned, received, pre.reshape(sources, count, pre.shape[1]))
        back_flat = returned.reshape(slot_total, width)
        taken = back_flat[index].astype(jnp.float32)
        moe = gate_pair[:, 0:1] * taken[:, 0] + gate_pair[:, 1:2] * taken[:, 1]
        outputs_list.append((residual + moe).astype(jnp.bfloat16).reshape(images_here, seq, width))
        grad_output = cotangent[micro].astype(jnp.float32).reshape(rows_dev, width)
        spread = jnp.sum(jnp.where(picks, gate_pair[None, :, :], 0.0), axis=2)
        grad_send = jnp.dot(spread, grad_output, precision=HIGH).astype(jnp.bfloat16)
        grad_received = lax.all_to_all(
            grad_send.reshape(experts, capacity, width),
            "expert",
            split_axis=0,
            concat_axis=0,
            tiled=True,
        )
        grad_rows_out = grad_received.reshape(slot_total, width)
        pre_rows = pre.reshape(slot_total, pre.shape[2])
        hidden_full, gelu_pull = jax.vjp(partial(jax.nn.gelu, approximate=False), pre_rows)
        hidden = hidden_full.astype(jnp.bfloat16)
        grad_down = grad_down + jnp.einsum(
            "rf,rd->fd", hidden, grad_rows_out, preferred_element_type=jnp.float32
        )
        grad_hidden = jnp.einsum(
            "rd,fd->rf", grad_rows_out, w_down, preferred_element_type=jnp.float32
        )
        grad_pre = gelu_pull(grad_hidden)[0].astype(jnp.bfloat16)
        rows_in = received.reshape(slot_total, width)
        grad_up = grad_up + jnp.einsum(
            "rf,rd->fd", grad_pre, rows_in, preferred_element_type=jnp.float32
        )
        grad_in = jnp.dot(grad_pre, w_up, preferred_element_type=jnp.float32).astype(jnp.bfloat16)
        grad_back = lax.all_to_all(
            grad_in.reshape(experts, capacity, width),
            "expert",
            split_axis=0,
            concat_axis=0,
            tiled=True,
        )
        pair_back = grad_back.reshape(slot_total, width)[index].astype(jnp.float32)
        grad_normed_two = pair_back[:, 0] + pair_back[:, 1]
        grad_two_rows, gain_two_grad, bias_two_grad = norm_backward(
            grad_normed_two, normed_two, inverse_two, norm_wide[2]
        )
        grad_residual = grad_output + grad_two_rows
        dense_again, norm_again = (
            lax.all_gather(dense_low, "dp", axis=0, tiled=True),
            lax.all_gather(norm_low, "dp", axis=1, tiled=True),
        )
        norm_again_wide = norm_again.astype(jnp.float32)
        grad_normed_one, grad_qkv_w, grad_out_w = attention_backward(
            grad_residual.reshape(images_here, seq, width),
            normed_one_low,
            dense_again[: 3 * width],
            dense_again[3 * width :],
            kept,
            HEADS,
        )
        grad_one_rows, gain_one_grad, bias_one_grad = norm_backward(
            grad_normed_one.reshape(rows_dev, width), normed_one, inverse_one, norm_again_wide[0]
        )
        input_list.append(
            (grad_residual + grad_one_rows).astype(jnp.bfloat16).reshape(images_here, seq, width)
        )
        grad_dense = grad_dense + jnp.concatenate([grad_qkv_w, grad_out_w], axis=0)
        grad_norm = grad_norm + jnp.stack(
            [gain_one_grad, bias_one_grad, gain_two_grad, bias_two_grad]
        )
    expert_terms = jnp.stack([grad_up, grad_down])[None]
    summed_dense, summed_norm, expert_grad = (
        lax.psum_scatter(
            grad_dense.astype(jnp.bfloat16), "dp", scatter_dimension=0, tiled=True
        ).astype(jnp.float32),
        lax.psum_scatter(
            grad_norm.astype(jnp.bfloat16), "dp", scatter_dimension=1, tiled=True
        ).astype(jnp.float32),
        lax.psum_scatter(
            expert_terms.astype(jnp.bfloat16), "dp", scatter_dimension=2, tiled=True
        ).astype(jnp.float32),
    )
    dense_grad, norm_grad = (
        lax.psum(summed_dense.astype(jnp.bfloat16), "expert").astype(jnp.float32),
        lax.psum(summed_norm.astype(jnp.bfloat16), "expert").astype(jnp.float32),
    )
    return (
        jnp.stack(outputs_list),
        jnp.stack(input_list),
        dense_grad,
        norm_grad,
        expert_grad,
    )


def shards(
    images,
    cotangent,
    gates,
    routes,
    slots,
    dense_master,
    dense_momentum,
    norm_master,
    norm_momentum,
    expert_master,
    expert_momentum,
):
    micro_count, images_here, seq, width = images.shape
    experts = lax.axis_size("expert")
    dp_count = lax.axis_size("dp")
    tokens_all = micro_count * images_here * seq * dp_count * experts
    lined = dense_master.shape[0] % 128 == 0 and expert_master.shape[2] % 128 == 0 and experts in (4, 8)
    lined = lined and dense_master.shape[0] == expert_master.shape[2] and micro_count == 2 and dp_count == 8
    vector_rate = LR_VECTOR * tokens_all ** (-0.5)
    if lined and images_here == 1 and width == 64 * HEADS:
        arrays = block(
            images, cotangent, gates, routes, dense_master, norm_master, expert_master, dense_momentum, expert_momentum
        )
        out, grad, *rest = finish(
            3 * width // dense_master.shape[0], vector_rate, *arrays,
            dense_momentum, norm_momentum, expert_momentum, dense_master, norm_master, expert_master,
        )
        return (out[:, None], grad[:, None], *rest)
    out, grad, dense_grad, norm_grad, expert_grad = block_plain(
        images, cotangent, gates, routes, slots, dense_master, norm_master, expert_master
    )
    norm_moment = DECAY * norm_momentum + norm_grad
    norm_new = norm_master - vector_rate * norm_moment
    expert_moment, dense_moment, expert_new, dense_new, expert_copy, dense_copy = muon(
        expert_grad, dense_grad, expert_momentum, dense_momentum, expert_master, dense_master
    )
    return (
        out,
        grad,
        dense_grad,
        norm_grad,
        expert_grad,
        dense_moment,
        norm_moment,
        expert_moment,
        dense_new,
        norm_new,
        expert_new,
        dense_copy,
        expert_copy,
    )


def solution(mesh):
    in_specs = (
        P(None, ("dp", "expert"), None, None),
        P(None, ("dp", "expert"), None, None),
        P(None, ("dp", "expert"), None, None),
        P(None, ("dp", "expert"), None, None),
        P(None, ("dp", "expert"), None, None),
        P("dp", None),
        P("dp", None),
        P(None, "dp"),
        P(None, "dp"),
        P("expert", None, "dp", None),
        P("expert", None, "dp", None),
    )
    out_specs = (
        P(None, ("dp", "expert"), None, None),
        P(None, ("dp", "expert"), None, None),
        P("dp", None),
        P(None, "dp"),
        P("expert", None, "dp", None),
        P("dp", None),
        P(None, "dp"),
        P("expert", None, "dp", None),
        P("dp", None),
        P(None, "dp"),
        P("expert", None, "dp", None),
        P("dp", None),
        P("expert", None, "dp", None),
    )
    return jax.shard_map(shards, mesh=mesh, in_specs=in_specs, out_specs=out_specs, check_vma=False)
```
